32 devices in a mesh: grp: 16 (over z, y, x), node: 2 (over core).
Axes of the slice: x: 2, y: 2, z: 4, core: 2. Of those that a mesh axis runs over, the one named last changes fastest.
Arguments:
- grad_out: bfloat16 [6144, 2048], P('grp', 'node'), may hold values from -12 to 12
- gate_prob: float32 [6144], P('grp'), may hold values from 0.05 to 1
- hidden: bfloat16 [6144, 7168], P('grp', 'node'), may hold values from -0.19921875 to 0.19921875
- w_down: bfloat16 [2048, 7168], P(None, 'node'), may hold values from -0.0625 to 0.0625
- slot_counts: int32 [16], P('grp'), may hold values from 0 to 384, as said below
Outputs:
- grad_hidden: bfloat16 [6144, 7168], P('grp', 'node')
- grad_weight: bfloat16 [2048, 7168], P('grp', 'node')
The draws below stay inside these ranges and needn't reach their ends.
Inputs may be any that keep to these rules, and one draw needn't show every extreme that they name: `slot_counts`: each count is a multiple of 128; in every draw some group's count is 384.
All inputs are finite; a program needn't handle non-finite values.
Results may differ from the reference program's by a relative error of at most 0.0057.
Values may be sent and summed in bfloat16 or wider, within the bound.
A program may use at most 128 MiB of HBM per device.

```python
import math
import jax
import jax.numpy as jnp
from jax import lax

D = 2048
FF = 7168
TILE_ROWS = 128
TILES = 3
CAP = 384
GROUPS = 16
ROWS = 6144


def draw_slot_counts(key, part):
    first_key, second_key, third_key = jax.random.split(key, 3)
    choose_full = jax.random.randint(first_key, (GROUPS,), 0, 4)
    light_tiles = jax.random.randint(second_key, (GROUPS,), 0, TILES // 2 + 1)
    tile_counts = jnp.where(choose_full == 0, TILES, light_tiles)
    full_group = jax.random.randint(third_key, (), 0, GROUPS)
    tile_counts = jnp.where(jnp.arange(GROUPS) == full_group, TILES, tile_counts)
    return (tile_counts * TILE_ROWS).astype(jnp.int32)


def raised(entries, rng, source, target, parts, factor):
    owner, partner = [(jnp.arange(entries.shape[position]) // (entries.shape[position] // parts)).reshape([-1 if axis == position else 1 for axis in range(entries.ndim)]) for position in (source, target)]
    chosen = jax.random.permutation(rng, parts)[partner]
    strong = (owner == chosen) | (owner == (partner + parts // 2) % parts)
    return jnp.where(strong, factor * entries, entries)


def shard_levels(own_key, extent, cuts, low, largest):
    def one(position, blocks):
        heights = jax.random.uniform(jax.random.fold_in(jax.random.fold_in(own_key, 6), position), (blocks,), jnp.float32, low / len(cuts), largest / len(cuts))
        return jnp.repeat(jnp.exp(heights), extent[position] // blocks).reshape((-1,) + (1,) * (len(extent) - position - 1))

    loudness = one(*cuts[0])
    for cut in cuts[1:]:
        loudness = loudness * one(*cut)
    return loudness


def gaussian(own_key, extent, width, most, shards=(), kind=jnp.bfloat16):
    values = width * jax.random.normal(own_key, extent, jnp.float32)
    if shards:
        values = values * shard_levels(own_key, extent, shards, -0.22, 0.18)
    return jnp.clip(values, -most, most).astype(kind)


def noise_with(key, shape, spread, limit, cuts, heavy, kind=jnp.bfloat16):
    array = spread * jax.random.normal(key, shape, jnp.float32)
    if cuts:
        array = array * shard_levels(key, shape, cuts, -0.22, 0.18)
    return jnp.clip(raised(array, jax.random.fold_in(key, 3), *heavy), -limit, limit).astype(kind)


def setup_inputs(seed: int = 0) -> dict:
    splits = jax.random.split(jax.random.key(seed), 6)
    return {
        "grad_out": noise_with(splits[0], (ROWS, D), 2.0, 12.0, ((0, 16), (1, 2)), (0, 1, 16, 2.0)),
        "gate_prob": jnp.clip(jnp.exp(math.log(1.0) - 2.9957323 * jax.random.uniform(splits[1], (ROWS,), jnp.float32) ** shard_levels(splits[1], (ROWS,), ((0, 16),), -0.2, 0.2)), 0.05, 1.0),
        "hidden": gaussian(splits[2], (ROWS, FF), 0.03, 0.19921875, ((0, 16), (1, 2))),
        "w_down": gaussian(splits[3], (D, FF), FF ** -0.5, 0.0625, ((1, 2),)),
        "slot_counts": draw_slot_counts(jax.random.fold_in(splits[5], 71), 0),
    }


def reference(grad_out, gate_prob, hidden, w_down, slot_counts):
    scaled = (gate_prob[:, None] * grad_out.astype(jnp.float32)).astype(jnp.bfloat16)
    slot_index = jnp.arange(ROWS, dtype=jnp.int32)
    group_index = (slot_index // CAP).astype(jnp.int32)
    live_slot = (slot_index % CAP) < slot_counts[group_index]
    masked = jnp.where(live_slot[:, None], scaled, jnp.zeros_like(scaled))
    grad_hidden = jnp.dot(masked, w_down, preferred_element_type=jnp.float32)
    grad_hidden = grad_hidden.astype(jnp.bfloat16)
    slot_blocks = masked.reshape(GROUPS, CAP, D)
    hidden_blocks = hidden.reshape(GROUPS, CAP, FF)

    def add_group(running, blocks):
        group_term = jnp.dot(blocks[0].T, blocks[1], preferred_element_type=jnp.float32)
        rounded = lax.optimization_barrier(group_term.astype(jnp.bfloat16))
        return running + rounded.astype(jnp.float32), None

    running, unused = lax.scan(add_group, jnp.zeros((D, FF), jnp.float32), (slot_blocks, hidden_blocks))
    return grad_hidden, running.astype(jnp.bfloat16)
```

```python
import functools

import jax
import jax.numpy as jnp
from jax import lax
from jax.experimental import pallas as pl
from jax.experimental.pallas import tpu as pltpu
from jax.sharding import PartitionSpec as P

MESH = pl.DeviceIdType.MESH
LANES = 128
WIDE = 2 * LANES
AHEAD = 1
HOP = 2
F32, BF16 = jnp.float32, jnp.bfloat16


def added(*terms):
    total = terms[0].astype(F32)
    for term in terms[1:]:
        total += term.astype(F32)
    return total.astype(BF16)


def kernel(
    dims, go_any, gate_ref, count_ref, hid_any, w_ref, gh_ref, gw_ref,
    go, g, shalf, scat, hid, wbuf, acc, ry, up, dn,
    gosem, hsem, wsem, gsend, grecv, ssend, srecv, xsend, xrecv, fsend, frecv,
    hsend, hrecv, ysend, yrecv, usend, urecv, dsend, drecv,
):
    nodes, depth, chunks = dims
    node = lax.axis_index("node")
    me = lax.axis_index("grp")
    mx, my, mz = me % 2, (me // 2) % 2, me // 4
    px, py = 1 - mx, 1 - my
    slots, half = go.shape
    rows = acc.shape[3]
    near = shalf.shape[1]
    last = depth - 1
    not_first, not_last = mz > 0, mz < last

    to_x = {"grp": me + 1 - 2 * mx}
    to_y = {"grp": me + 2 - 4 * my}
    to_up, to_down = {"grp": me + 4}, {"grp": me - 4}

    barrier = pltpu.get_barrier_semaphore()

    def greet(target):
        pl.semaphore_signal(barrier, inc=1, device_id=target, device_id_type=MESH)

    greet(to_x)
    greet(to_y)
    for off in range(1, nodes):
        greet({"node": (node + off) % nodes})

    @pl.when(not_first)
    def _():
        greet(to_down)

    @pl.when(not_last)
    def _():
        greet(to_up)

    def columns(c):
        return pl.ds(pl.multiple_of(c * WIDE, WIDE), WIDE)

    def w_copy(c, slot):
        return pltpu.make_async_copy(w_ref.at[:, columns(c)], wbuf.at[slot], wsem.at[slot])

    own = pl.ds(0, slots)
    theirs = pl.ds(slots, slots)
    take_hidden = pltpu.make_async_copy(hid_any, hid.at[own], hsem)
    take_grad = pltpu.make_async_copy(go_any, go, gosem)
    take_grad.start()
    take_hidden.start()
    w_copy(0, 0).start()

    def remote(src, dst, ssem, rsem, target):
        return pltpu.make_async_remote_copy(
            src_ref=src, dst_ref=dst, send_sem=ssem, recv_sem=rsem,
            device_id=target, device_id_type=MESH,
        )

    def peer(off):
        return {"node": (node + off) % nodes}

    def swap_scaled(off):
        return remote(g.at[node], g.at[node], gsend.at[off], grecv.at[off], peer(off))

    def swap_turned(off):
        dst = scat.at[pl.ds(node * near, near), :, :, own]
        return remote(shalf.at[mx], dst, ssend.at[off], srecv.at[off], peer(off))

    def x_scaled(i):
        dst = scat.at[node * near + i, :, :, theirs]
        return remote(shalf.at[px, i], dst, xsend.at[i], xrecv.at[i], to_x)

    def forward(off, i):
        ref = scat.at[node * near + i, :, :, theirs]
        return remote(ref, ref, fsend.at[off, i], frecv.at[off, i], peer(off))

    def x_hidden(c):
        return remote(
            hid.at[own, columns(c)], hid.at[theirs, columns(c)],
            hsend.at[c], hrecv.at[c], to_x,
        )

    def y_copy(c, d):
        return remote(acc.at[c, d, py], ry.at[c, d], ysend.at[c, d], yrecv.at[c, d], to_y)

    def z_copy(c, d, rising, both):
        if both:
            pick = lambda ref: ref.at[c, d]
        else:
            pick = lambda ref: ref.at[c, d, my]
        if rising:
            return remote(pick(acc), pick(up), usend.at[c, d], urecv.at[c, d], to_up)
        return remote(pick(acc), pick(dn), dsend.at[c, d], drecv.at[c, d], to_down)

    def late(c):
        return c % 2 == 0

    def each_d(run, least=1):
        for k in range(last, least - 1, -1):
            @pl.when(mz + k <= last)
            def _():
                run(mz + k, k)

            @pl.when(mz - k >= 0)
            def _():
                run(mz - k, k)

    pl.semaphore_wait(
        barrier, 1 + nodes + not_first.astype(jnp.int32) + not_last.astype(jnp.int32)
    )
    take_hidden.wait()
    x_hidden(0).start()
    take_grad.wait()

    live = lax.broadcasted_iota(jnp.int32, (LANES, slots), 1) < count_ref[0]
    gate = jnp.broadcast_to(gate_ref[...].reshape(1, slots), (LANES, slots))
    gate = jnp.where(live, gate, 0.0).T
    for i in range(half // LANES):
        cols = pl.ds(i * LANES, LANES)
        scaled = (go[:, cols].astype(F32) * gate).astype(BF16)
        g[node, :, cols] = scaled
        turned = scaled.T
        for j in range(LANES // rows):
            b = i * (LANES // rows) + j
            shalf[b % 2, b // 4, (b // 2) % 2] = turned[j * rows : (j + 1) * rows]
    for i in range(near):
        x_scaled(i).start()
    for off in range(1, nodes):
        swap_turned(off).start()
        swap_scaled(off).start()
    lax.fori_loop(1, chunks, lambda c, carry: (x_hidden(c).start(), carry)[1], 0)
    for i in range(near):
        scat[node * near + i, :, :, :slots] = shalf[mx, i]
    for off in range(1, nodes):
        swap_scaled(off).wait_recv()

    def make_hidden(c):
        slot = c % 2
        w_copy(c, slot).wait()

        @pl.when(c + 1 < chunks)
        def _():
            w_copy(c + 1, 1 - slot).start()

        total = jnp.dot(g[0], wbuf[slot, :half, :], preferred_element_type=F32)
        for i in range(1, nodes):
            total += jnp.dot(
                g[i], wbuf[slot, i * half : (i + 1) * half, :], preferred_element_type=F32
            )
        gh_ref[:, columns(c)] = total.astype(BF16)

    def hidden_range(start, stop):
        lax.fori_loop(start, stop, lambda c, carry: (make_hidden(c), carry)[1], 0)

    done = 0
    for i in range(near):
        until = chunks * (i + 2) // (near + 2)
        hidden_range(done, until)
        done = until
        x_scaled(i).wait_recv()
        for off in range(1, nodes):
            forward(off, i).start()
    hidden_range(done, chunks)
    for off in range(1, nodes):
        swap_turned(off).wait_recv()
        for i in range(near):
            forward(off, i).wait_recv()

    def make(c):
        x_hidden(c).wait_recv()
        units = hid[:, columns(c)]

        def two(j, carry):
            part = scat[pl.ds(2 * j, 2)].reshape(4 * rows, 2 * slots)
            product = jnp.dot(part, units, preferred_element_type=F32).astype(BF16)
            acc[c, pl.ds(2 * j, 2)] = product.reshape(2, 2, rows, WIDE)
            return carry

        lax.fori_loop(0, depth // 2, two, 0)

        def send(d, k):
            if k > 1:
                y_copy(c, d).start()
            else:
                @pl.when(jnp.logical_not(late(c)))
                def _():
                    y_copy(c, d).start()

        each_d(send)

    def pass_on(c, rising):
        inside = not_first if rising else not_last
        into = up if rising else dn

        def single(d):
            y_copy(c, d).wait_recv()

            @pl.when(inside)
            def _():
                z_copy(c, d, rising, False).wait_recv()
                acc[c, d, my] = added(acc[c, d, my], ry[c, d], into[c, d, my])

            @pl.when(jnp.logical_not(inside))
            def _():
                acc[c, d, my] = added(acc[c, d, my], ry[c, d])

            z_copy(c, d, rising, False).start()

        def double(d):
            @pl.when(inside)
            def _():
                z_copy(c, d, rising, False).wait_recv()
                acc[c, d, my] = added(acc[c, d, my], into[c, d, my])

            z_copy(c, d, rising, True).start()

        for k in range(last, 0, -1):
            d = mz + k if rising else mz - k

            @pl.when((d <= last) if rising else (d >= 0))
            def _():
                if k > 1:
                    single(d)
                else:
                    @pl.when(late(c))
                    def _():
                        double(d)

                    @pl.when(jnp.logical_not(late(c)))
                    def _():
                        single(d)

    def settle(c):
        @pl.when(late(c))
        def _():
            @pl.when(not_first)
            def _():
                z_copy(c, mz, True, True).wait_recv()
                acc[c, mz] = added(acc[c, mz], up[c, mz])

            @pl.when(not_last)
            def _():
                z_copy(c, mz, False, True).wait_recv()
                acc[c, mz] = added(acc[c, mz], dn[c, mz])

        y_copy(c, mz).start()

    def finish(c):
        y_copy(c, mz).wait_recv()
        cols = columns(c)

        @pl.when(late(c))
        def _():
            gw_ref[:, cols] = added(acc[c, mz, my], ry[c, mz])

        @pl.when(jnp.logical_not(late(c)))
        def _():
            @pl.when(not_first)
            def _():
                z_copy(c, mz, True, False).wait_recv()

            @pl.when(not_last)
            def _():
                z_copy(c, mz, False, False).wait_recv()

            @pl.when(mz == 0)
            def _():
                gw_ref[:, cols] = added(acc[c, mz, my], ry[c, mz], dn[c, mz, my])

            @pl.when(mz == last)
            def _():
                gw_ref[:, cols] = added(acc[c, mz, my], ry[c, mz], up[c, mz, my])

            @pl.when(not_first & not_last)
            def _():
                gw_ref[:, cols] = added(
                    acc[c, mz, my], ry[c, mz], up[c, mz, my], dn[c, mz, my]
                )

    def within(c, run):
        @pl.when((c >= 0) & (c < chunks))
        def _():
            run(c)

    def step(t, carry):
        within(t, make)

        @pl.when(not_last)
        def _():
            within(t - AHEAD - HOP * mz, lambda c: pass_on(c, True))

        @pl.when(not_first)
        def _():
            within(t - AHEAD - HOP * (last - mz), lambda c: pass_on(c, False))

        within(t - AHEAD - HOP * last, settle)
        within(t - AHEAD - HOP * last - 1, finish)
        return carry

    lax.fori_loop(0, chunks + AHEAD + HOP * last + 1, step, 0)

    for off in range(1, nodes):
        swap_turned(off).wait_send()
        swap_scaled(off).wait_send()
        for i in range(near):
            forward(off, i).wait_send()
    for i in range(near):
        x_scaled(i).wait_send()

    def drain(c, carry):
        x_hidden(c).wait_send()
        y_copy(c, mz).wait_send()

        def one(d, k):
            if k > 1:
                y_copy(c, d).wait_send()
            else:
                @pl.when(jnp.logical_not(late(c)))
                def _():
                    y_copy(c, d).wait_send()

        each_d(one)
        for k in range(1, depth):
            for rising in (True, False):
                d = mz + k if rising else mz - k

                @pl.when((d <= last) if rising else (d >= 0))
                def _():
                    if k > 1:
                        z_copy(c, d, rising, False).wait_send()
                    else:
                        @pl.when(late(c))
                        def _():
                            z_copy(c, d, rising, True).wait_send()

                        @pl.when(jnp.logical_not(late(c)))
                        def _():
                            z_copy(c, d, rising, False).wait_send()
        return carry

    lax.fori_loop(0, chunks, drain, 0)


def body(grad_out, gate_prob, hidden, w_down, slot_counts):
    slots, half = grad_out.shape
    nodes, groups = lax.axis_size("node"), lax.axis_size("grp")
    depth = groups // 4
    near = depth // nodes
    model = w_down.shape[0]
    rows = model // groups
    units = hidden.shape[1]
    chunks = -(-units // WIDE)
    extra = chunks * WIDE - units
    if extra:
        hidden = jnp.pad(hidden, ((0, 0), (0, extra)))
        w_down = jnp.pad(w_down, ((0, 0), (0, extra)))
    dma = pltpu.SemaphoreType.DMA
    vmem = pl.BlockSpec(memory_space=pltpu.VMEM)
    smem = pl.BlockSpec(memory_space=pltpu.SMEM)
    anywhere = pl.BlockSpec(memory_space=pl.ANY)
    grad_hidden, grad_weight = pl.pallas_call(
        functools.partial(kernel, (nodes, depth, chunks)),
        out_shape=(
            pltpu.VMEM((slots, chunks * WIDE), BF16),
            pltpu.VMEM((rows, chunks * WIDE), BF16),
        ),
        in_specs=[anywhere, vmem, smem, anywhere, anywhere],
        out_specs=(vmem, vmem),
        scratch_shapes=[
            pltpu.VMEM((slots, half), BF16),
            pltpu.VMEM((nodes, slots, half), BF16),
            pltpu.VMEM((2, near, 2, rows, slots), BF16),
            pltpu.VMEM((depth, 2, rows, 2 * slots), BF16),
            pltpu.VMEM((2 * slots, chunks * WIDE), BF16),
            pltpu.VMEM((2, model, WIDE), BF16),
            pltpu.VMEM((chunks, depth, 2, rows, WIDE), BF16),
            pltpu.VMEM((chunks, depth, rows, WIDE), BF16),
            pltpu.VMEM((chunks, depth, 2, rows, WIDE), BF16),
            pltpu.VMEM((chunks, depth, 2, rows, WIDE), BF16),
            dma(()),
            dma(()),
            dma((2,)),
            dma((nodes,)),
            dma((nodes,)),
            dma((nodes,)),
            dma((nodes,)),
            dma((near,)),
            dma((near,)),
            dma((nodes, near)),
            dma((nodes, near)),
            dma((chunks,)),
            dma((chunks,)),
            dma((chunks, depth)),
            dma((chunks, depth)),
            dma((chunks, depth)),
            dma((chunks, depth)),
            dma((chunks, depth)),
            dma((chunks, depth)),
        ],
        compiler_params=pltpu.CompilerParams(
            collective_id=0, has_side_effects=True, vmem_limit_bytes=54 * 1024 * 1024
        ),
    )(grad_out, gate_prob, slot_counts, hidden, w_down)
    return grad_hidden[:, :units], grad_weight[:, :units]


def solution(mesh):
    return jax.shard_map(
        body,
        mesh=mesh,
        in_specs=(P("grp", "node"), P("grp"), P("grp", "node"), P(None, "node"), P("grp")),
        out_specs=(P("grp", "node"), P("grp", "node")),
        check_vma=False,
    )
```

```python
import functools

import jax
import jax.numpy as jnp
from jax import lax
from jax.experimental import pallas as pl
from jax.experimental.pallas import tpu as pltpu
from jax.sharding import PartitionSpec as P

MESH = pl.DeviceIdType.MESH
LANES = 128
WIDE = 2 * LANES
AHEAD = 1
HOP = 1
DEFER = 1
NEAR = 2
EARLY = 3
F32, BF16 = jnp.float32, jnp.bfloat16


def added(*terms):
    total = terms[0].astype(F32)
    for term in terms[1:]:
        total += term.astype(F32)
    return total.astype(BF16)


def kernel(
    dims, go_any, gate_ref, count_ref, hid_any, w_ref, gh_ref, gw_ref,
    go, g, shalf, scat, hid, wbuf, acc, ry, up, dn,
    gosem, hsem, wsem, gsend, grecv, ssend, srecv, xsend, xrecv, fsend, frecv,
    hsend, hrecv, ysend, yrecv, usend, urecv, dsend, drecv,
):
    nodes, depth, chunks = dims
    node = lax.axis_index("node")
    me = lax.axis_index("grp")
    mx, my, mz = me % 2, (me // 2) % 2, me // 4
    px, py = 1 - mx, 1 - my
    slots, half = go.shape
    rows = acc.shape[3]
    near = shalf.shape[1]
    last = depth - 1
    not_first, not_last = mz > 0, mz < last

    to_x = {"grp": me + 1 - 2 * mx}
    to_y = {"grp": me + 2 - 4 * my}
    to_up, to_down = {"grp": me + 4}, {"grp": me - 4}

    barrier = pltpu.get_barrier_semaphore()

    def greet(target):
        pl.semaphore_signal(barrier, inc=1, device_id=target, device_id_type=MESH)

    greet(to_x)
    greet(to_y)
    for off in range(1, nodes):
        greet({"node": (node + off) % nodes})

    @pl.when(not_first)
    def _():
        greet(to_down)

    @pl.when(not_last)
    def _():
        greet(to_up)

    def columns(c):
        return pl.ds(pl.multiple_of(c * WIDE, WIDE), WIDE)

    def w_copy(c, slot):
        return pltpu.make_async_copy(w_ref.at[:, columns(c)], wbuf.at[slot], wsem.at[slot])

    own = pl.ds(0, slots)
    theirs = pl.ds(slots, slots)
    take_hidden = pltpu.make_async_copy(hid_any, hid.at[own], hsem)
    take_grad = pltpu.make_async_copy(go_any, go, gosem)
    take_grad.start()
    take_hidden.start()
    w_copy(0, 0).start()

    def remote(src, dst, ssem, rsem, target):
        return pltpu.make_async_remote_copy(
            src_ref=src, dst_ref=dst, send_sem=ssem, recv_sem=rsem,
            device_id=target, device_id_type=MESH,
        )

    def peer(off):
        return {"node": (node + off) % nodes}

    def swap_scaled(off):
        return remote(g.at[node], g.at[node], gsend.at[off], grecv.at[off], peer(off))

    def swap_turned(off):
        dst = scat.at[pl.ds(node * near, near), :, :, own]
        return remote(shalf.at[mx], dst, ssend.at[off], srecv.at[off], peer(off))

    def nth(owner, i):
        return jnp.where(2 * owner < nodes, i, near - 1 - i)

    def x_scaled(i):
        j = nth(node, i)
        dst = scat.at[node * near + j, :, :, theirs]
        return remote(shalf.at[px, j], dst, xsend.at[i], xrecv.at[i], to_x)

    def forward(off, i):
        ref = scat.at[node * near + nth(node, i), :, :, theirs]
        return remote(ref, ref, fsend.at[off, i], frecv.at[off, i], peer(off))

    def x_hidden(c):
        return remote(
            hid.at[own, columns(c)], hid.at[theirs, columns(c)],
            hsend.at[c], hrecv.at[c], to_x,
        )

    def y_copy(c, d):
        return remote(acc.at[c, d, py], ry.at[c, d], ysend.at[c, d], yrecv.at[c, d], to_y)

    def z_copy(c, d, rising, both):
        if both:
            pick = lambda ref: ref.at[c, d]
        else:
            pick = lambda ref: ref.at[c, d, my]
        if rising:
            return remote(pick(acc), pick(up), usend.at[c, d], urecv.at[c, d], to_up)
        return remote(pick(acc), pick(dn), dsend.at[c, d], drecv.at[c, d], to_down)

    def late(c):
        return (c % 2 == 1) & (c < chunks - 3)

    def each_d(run, least=1):
        for k in range(last, least - 1, -1):
            @pl.when(mz + k <= last)
            def _():
                run(mz + k, k)

            @pl.when(mz - k >= 0)
            def _():
                run(mz - k, k)

    pl.semaphore_wait(
        barrier, 1 + nodes + not_first.astype(jnp.int32) + not_last.astype(jnp.int32)
    )
    take_hidden.wait()
    x_hidden(0).start()
    take_grad.wait()

    live = lax.broadcasted_iota(jnp.int32, (LANES, slots), 1) < count_ref[0]
    gate = jnp.broadcast_to(gate_ref[...].reshape(1, slots), (LANES, slots))
    gate = jnp.where(live, gate, 0.0).T
    for i in range(half // LANES):
        cols = pl.ds(i * LANES, LANES)
        scaled = (go[:, cols].astype(F32) * gate).astype(BF16)
        g[node, :, cols] = scaled
        turned = scaled.T
        for j in range(LANES // rows):
            b = i * (LANES // rows) + j
            shalf[b % 2, b // 4, (b // 2) % 2] = turned[j * rows : (j + 1) * rows]
    for i in range(near):
        x_scaled(i).start()
    for off in range(1, nodes):
        swap_turned(off).start()
        swap_scaled(off).start()
    lax.fori_loop(1, chunks, lambda c, carry: (x_hidden(c).start(), carry)[1], 0)
    for i in range(near):
        scat[node * near + i, :, :, :slots] = shalf[mx, i]
    for off in range(1, nodes):
        swap_scaled(off).wait_recv()

    def make_hidden(c):
        slot = c % 2
        w_copy(c, slot).wait()

        @pl.when(c + 1 < chunks)
        def _():
            w_copy(c + 1, 1 - slot).start()

        total = jnp.dot(g[0], wbuf[slot, :half, :], preferred_element_type=F32)
        for i in range(1, nodes):
            total += jnp.dot(
                g[i], wbuf[slot, i * half : (i + 1) * half, :], preferred_element_type=F32
            )
        gh_ref[:, columns(c)] = total.astype(BF16)

    def hidden_range(start, stop):
        lax.fori_loop(start, stop, lambda c, carry: (make_hidden(c), carry)[1], 0)

    def send(c, d):
        k = jnp.abs(d - mz)

        @pl.when((k > 1) | ((k == 1) & jnp.logical_not(late(c))))
        def _():
            y_copy(c, d).start()

    def make_first(owner, i):
        d = owner * near + nth(owner, i)
        part = scat[d].reshape(2 * rows, 2 * slots)
        product = jnp.dot(part, hid[:, :WIDE], preferred_element_type=F32).astype(BF16)
        acc[0, d] = product.reshape(2, rows, WIDE)
        send(0, d)

    done = 0
    for i in range(near):
        until = chunks * (i + near) // (2 * near)
        hidden_range(done, until)
        done = until
        if i == 0:
            for off in range(1, nodes):
                swap_turned(off).wait_recv()
        x_scaled(i).wait_recv()
        for off in range(1, nodes):
            forward(off, i).start()
        if i == 0:
            x_hidden(0).wait_recv()
        make_first(node, i)
        for off in range(1, nodes):
            forward(off, i).wait_recv()
            make_first((node + nodes - off) % nodes, i)

    def make(c):
        x_hidden(c).wait_recv()
        units = hid[:, columns(c)]

        def two(j, carry):
            part = scat[pl.ds(2 * j, 2)].reshape(4 * rows, 2 * slots)
            product = jnp.dot(part, units, preferred_element_type=F32).astype(BF16)
            acc[c, pl.ds(2 * j, 2)] = product.reshape(2, 2, rows, WIDE)
            return carry

        lax.fori_loop(0, depth // 2, two, 0)

        @pl.when(late(c) & (c < EARLY))
        def _():
            @pl.when(mz == 0)
            def _():
                hand_over(c, True)

            @pl.when(mz == last)
            def _():
                hand_over(c, False)

        each_d(lambda d, k: send(c, d))

    def pass_on(c, rising):
        inside = not_first if rising else not_last
        into = up if rising else dn

        def single(d):
            y_copy(c, d).wait_recv()

            @pl.when(inside)
            def _():
                z_copy(c, d, rising, False).wait_recv()
                acc[c, d, my] = added(acc[c, d, my], ry[c, d], into[c, d, my])

            @pl.when(jnp.logical_not(inside))
            def _():
                acc[c, d, my] = added(acc[c, d, my], ry[c, d])

            z_copy(c, d, rising, False).start()

        for k in range(last, 1, -1):
            d = mz + k if rising else mz - k

            @pl.when((d <= last) if rising else (d >= 0))
            def _():
                single(d)

    def hand_over(c, rising):
        inside = not_first if rising else not_last
        into = up if rising else dn
        d = mz + 1 if rising else mz - 1

        @pl.when(inside)
        def _():
            z_copy(c, d, rising, False).wait_recv()
            acc[c, d, my] = added(acc[c, d, my], into[c, d, my])

        @pl.when(late(c))
        def _():
            z_copy(c, d, rising, True).start()

        @pl.when(jnp.logical_not(late(c)))
        def _():
            y_copy(c, d).wait_recv()
            acc[c, d, my] = added(acc[c, d, my], ry[c, d])
            z_copy(c, d, rising, False).start()

    def settle(c):
        @pl.when(late(c))
        def _():
            @pl.when(not_first)
            def _():
                z_copy(c, mz, True, True).wait_recv()
                acc[c, mz] = added(acc[c, mz], up[c, mz])

            @pl.when(not_last)
            def _():
                z_copy(c, mz, False, True).wait_recv()
                acc[c, mz] = added(acc[c, mz], dn[c, mz])

            y_copy(c, mz).start()

    def finish(c):
        y_copy(c, mz).wait_recv()
        cols = columns(c)

        @pl.when(late(c))
        def _():
            gw_ref[:, cols] = added(acc[c, mz, my], ry[c, mz])

        @pl.when(jnp.logical_not(late(c)))
        def _():
            @pl.when(not_first)
            def _():
                z_copy(c, mz, True, False).wait_recv()

            @pl.when(not_last)
            def _():
                z_copy(c, mz, False, False).wait_recv()

            @pl.when(mz == 0)
            def _():
                gw_ref[:, cols] = added(acc[c, mz, my], ry[c, mz], dn[c, mz, my])

            @pl.when(mz == last)
            def _():
                gw_ref[:, cols] = added(acc[c, mz, my], ry[c, mz], up[c, mz, my])

            @pl.when(not_first & not_last)
            def _():
                gw_ref[:, cols] = added(
                    acc[c, mz, my], ry[c, mz], up[c, mz, my], dn[c, mz, my]
                )

    def within(c, run):
        @pl.when((c >= 0) & (c < chunks))
        def _():
            run(c)

    settled = AHEAD + HOP * last + DEFER + 1

    def step(t, carry):
        @pl.when((t > 0) & (t < chunks))
        def _():
            make(t)

        @pl.when(t + done < chunks)
        def _():
            make_hidden(t + done)

        rise = t - AHEAD - HOP * mz
        fall = t - AHEAD - HOP * (last - mz)

        @pl.when(not_last)
        def _():
            within(rise, lambda c: pass_on(c, True))

        @pl.when(not_first)
        def _():
            within(fall, lambda c: pass_on(c, False))

        def early(c, inside):
            return late(c) & (c < EARLY) & jnp.logical_not(inside)

        @pl.when(not_last & jnp.logical_not(early(rise - DEFER, not_first)))
        def _():
            within(rise - DEFER, lambda c: hand_over(c, True))

        @pl.when(not_first & jnp.logical_not(early(fall - DEFER, not_last)))
        def _():
            within(fall - DEFER, lambda c: hand_over(c, False))

        within(t - settled, settle)

        @pl.when((t >= NEAR) & (t < chunks + NEAR) & jnp.logical_not(late(t - NEAR)))
        def _():
            y_copy(t - NEAR, mz).start()

        within(t - settled - 2, finish)
        return carry

    lax.fori_loop(0, chunks + settled + 2, step, 0)

    for off in range(1, nodes):
        swap_turned(off).wait_send()
        swap_scaled(off).wait_send()
        for i in range(near):
            forward(off, i).wait_send()
    for i in range(near):
        x_scaled(i).wait_send()

    def drain(c, carry):
        x_hidden(c).wait_send()
        y_copy(c, mz).wait_send()

        def one(d, k):
            if k > 1:
                y_copy(c, d).wait_send()
            else:
                @pl.when(jnp.logical_not(late(c)))
                def _():
                    y_copy(c, d).wait_send()

        each_d(one)
        for k in range(1, depth):
            for rising in (True, False):
                d = mz + k if rising else mz - k

                @pl.when((d <= last) if rising else (d >= 0))
                def _():
                    if k > 1:
                        z_copy(c, d, rising, False).wait_send()
                    else:
                        @pl.when(late(c))
                        def _():
                            z_copy(c, d, rising, True).wait_send()

                        @pl.when(jnp.logical_not(late(c)))
                        def _():
                            z_copy(c, d, rising, False).wait_send()
        return carry

    lax.fori_loop(0, chunks, drain, 0)


def body(grad_out, gate_prob, hidden, w_down, slot_counts):
    slots, half = grad_out.shape
    nodes, groups = lax.axis_size("node"), lax.axis_size("grp")
    depth = groups // 4
    near = depth // nodes
    model = w_down.shape[0]
    rows = model // groups
    units = hidden.shape[1]
    chunks = -(-units // WIDE)
    extra = chunks * WIDE - units
    if extra:
        hidden = jnp.pad(hidden, ((0, 0), (0, extra)))
        w_down = jnp.pad(w_down, ((0, 0), (0, extra)))
    dma = pltpu.SemaphoreType.DMA
    vmem = pl.BlockSpec(memory_space=pltpu.VMEM)
    smem = pl.BlockSpec(memory_space=pltpu.SMEM)
    anywhere = pl.BlockSpec(memory_space=pl.ANY)
    grad_hidden, grad_weight = pl.pallas_call(
        functools.partial(kernel, (nodes, depth, chunks)),
        out_shape=(
            pltpu.VMEM((slots, chunks * WIDE), BF16),
            pltpu.VMEM((rows, chunks * WIDE), BF16),
        ),
        in_specs=[anywhere, vmem, smem, anywhere, anywhere],
        out_specs=(vmem, vmem),
        scratch_shapes=[
            pltpu.VMEM((slots, half), BF16),
            pltpu.VMEM((nodes, slots, half), BF16),
            pltpu.VMEM((2, near, 2, rows, slots), BF16),
            pltpu.VMEM((depth, 2, rows, 2 * slots), BF16),
            pltpu.VMEM((2 * slots, chunks * WIDE), BF16),
            pltpu.VMEM((2, model, WIDE), BF16),
            pltpu.VMEM((chunks, depth, 2, rows, WIDE), BF16),
            pltpu.VMEM((chunks, depth, rows, WIDE), BF16),
            pltpu.VMEM((chunks, depth, 2, rows, WIDE), BF16),
            pltpu.VMEM((chunks, depth, 2, rows, WIDE), BF16),
            dma(()),
            dma(()),
            dma((2,)),
            dma((nodes,)),
            dma((nodes,)),
            dma((nodes,)),
            dma((nodes,)),
            dma((near,)),
            dma((near,)),
            dma((nodes, near)),
            dma((nodes, near)),
            dma((chunks,)),
            dma((chunks,)),
            dma((chunks, depth)),
            dma((chunks, depth)),
            dma((chunks, depth)),
            dma((chunks, depth)),
            dma((chunks, depth)),
            dma((chunks, depth)),
        ],
        compiler_params=pltpu.CompilerParams(
            collective_id=0, has_side_effects=True, vmem_limit_bytes=54 * 1024 * 1024
        ),
    )(grad_out, gate_prob, slot_counts, hidden, w_down)
    return grad_hidden[:, :units], grad_weight[:, :units]


def solution(mesh):
    return jax.shard_map(
        body,
        mesh=mesh,
        in_specs=(P("grp", "node"), P("grp"), P("grp", "node"), P(None, "node"), P("grp")),
        out_specs=(P("grp", "node"), P("grp", "node")),
        check_vma=False,
    )
```

```python
import functools
from types import SimpleNamespace

import jax
import jax.numpy as jnp
from jax import lax
from jax.experimental import pallas as pl
from jax.experimental.pallas import tpu as pltpu
from jax.sharding import PartitionSpec as P

MESH = pl.DeviceIdType.MESH
LANES = 128
WIDE = 2 * LANES
AHEAD = 1
HOP = 1
DEFER = 1
NEAR = 3
LAST = 3
F32, BF16 = jnp.float32, jnp.bfloat16


def added(*terms):
    total = terms[0].astype(F32)
    for term in terms[1:]:
        total += term.astype(F32)
    return total.astype(BF16)


def kernel(
    dims, go_any, gate_ref, count_ref, hid_any, w_ref, gh_ref, gw_ref,
    go, g, sall, scat, hid, wbuf, acc, ry, up, dn, qacc, qry, qup, qdn, qrx,
    gosem, hsem, wsem, gsend, grecv, ssend, srecv, xsend, xrecv, fsend, frecv,
    hsend, hrecv, ysend, yrecv, usend, urecv, dsend, drecv,
    qysend, qyrecv, qusend, qurecv, qdsend, qdrecv, qxsend, qxrecv,
):
    nodes, depth, total_chunks = dims
    chunks = total_chunks - 1
    node = lax.axis_index("node")
    me = lax.axis_index("grp")
    mx, my, mz = me % 2, (me // 2) % 2, me // 4
    px, py = 1 - mx, 1 - my
    slots, half = go.shape
    rows = acc.shape[3]
    near = depth // nodes
    last = depth - 1
    not_first, not_last = mz > 0, mz < last

    to_x = {"grp": me + 1 - 2 * mx}
    to_y = {"grp": me + 2 - 4 * my}
    to_up, to_down = {"grp": me + 4}, {"grp": me - 4}

    barrier = pltpu.get_barrier_semaphore()

    def greet(target):
        pl.semaphore_signal(barrier, inc=1, device_id=target, device_id_type=MESH)

    greet(to_x)
    greet(to_y)
    for off in range(1, nodes):
        greet({"node": (node + off) % nodes})

    @pl.when(not_first)
    def _():
        greet(to_down)

    @pl.when(not_last)
    def _():
        greet(to_up)

    def columns(c):
        return pl.ds(pl.multiple_of(c * WIDE, WIDE), WIDE)

    def w_copy(c, slot):
        return pltpu.make_async_copy(w_ref.at[:, columns(c)], wbuf.at[slot], wsem.at[slot])

    own = pl.ds(0, slots)
    theirs = pl.ds(slots, slots)
    take_hidden = pltpu.make_async_copy(hid_any, hid.at[own], hsem)
    take_grad = pltpu.make_async_copy(go_any, go, gosem)
    take_grad.start()
    take_hidden.start()
    w_copy(0, 0).start()

    def remote(src, dst, ssem, rsem, target):
        return pltpu.make_async_remote_copy(
            src_ref=src, dst_ref=dst, send_sem=ssem, recv_sem=rsem,
            device_id=target, device_id_type=MESH,
        )

    def peer(off):
        return {"node": (node + off) % nodes}

    def swap_scaled(off):
        return remote(g.at[node], g.at[node], gsend.at[off], grecv.at[off], peer(off))

    def swap_turned(off):
        ref = sall.at[pl.ds(node * near, near)]
        return remote(ref, ref, ssend.at[off], srecv.at[off], peer(off))

    def nth(owner, i):
        return jnp.where(2 * owner < nodes, i, near - 1 - i)

    def x_scaled(i):
        d = node * near + nth(node, i)
        dst = scat.at[d, :, :, theirs]
        return remote(sall.at[d, :, px], dst, xsend.at[i], xrecv.at[i], to_x)

    def forward(off, i):
        ref = scat.at[node * near + nth(node, i), :, :, theirs]
        return remote(ref, ref, fsend.at[off, i], frecv.at[off, i], peer(off))

    def x_hidden(c):
        return remote(
            hid.at[own, columns(c)], hid.at[theirs, columns(c)],
            hsend.at[c], hrecv.at[c], to_x,
        )

    def late(c):
        return (c % 2 == 1) & (c > 2) & (c < chunks - 3)

    main = SimpleNamespace(
        acc=acc, ry=ry, up=up, dn=dn, late=late, ysend=ysend, yrecv=yrecv,
        usend=usend, urecv=urecv, dsend=dsend, drecv=drecv,
    )
    lone = SimpleNamespace(
        acc=qacc, ry=qry, up=qup, dn=qdn, late=lambda c: c < 0, ysend=qysend, yrecv=qyrecv,
        usend=qusend, urecv=qurecv, dsend=qdsend, drecv=qdrecv,
    )

    def y_copy(f, c, d):
        return remote(
            f.acc.at[c, d, py], f.ry.at[c, d], f.ysend.at[c, d], f.yrecv.at[c, d], to_y
        )

    def z_copy(f, c, d, rising, both):
        if both:
            pick = lambda ref: ref.at[c, d]
        else:
            pick = lambda ref: ref.at[c, d, my]
        if rising:
            return remote(
                pick(f.acc), pick(f.up), f.usend.at[c, d], f.urecv.at[c, d], to_up
            )
        return remote(
            pick(f.acc), pick(f.dn), f.dsend.at[c, d], f.drecv.at[c, d], to_down
        )

    def each_d(run, least=1):
        for k in range(last, least - 1, -1):
            @pl.when(mz + k <= last)
            def _():
                run(mz + k, k)

            @pl.when(mz - k >= 0)
            def _():
                run(mz - k, k)

    pl.semaphore_wait(
        barrier, 1 + nodes + not_first.astype(jnp.int32) + not_last.astype(jnp.int32)
    )
    take_hidden.wait()
    x_hidden(0).start()
    take_grad.wait()

    live = lax.broadcasted_iota(jnp.int32, (LANES, slots), 1) < count_ref[0]
    gate = jnp.broadcast_to(gate_ref[...].reshape(1, slots), (LANES, slots))
    gate = jnp.where(live, gate, 0.0).T
    for i in range(half // LANES):
        cols = pl.ds(i * LANES, LANES)
        scaled = (go[:, cols].astype(F32) * gate).astype(BF16)
        g[node, :, cols] = scaled
        turned = scaled.T
        for j in range(LANES // rows):
            b = i * (LANES // rows) + j
            sall[node * near + b // 4, (b // 2) % 2, b % 2] = turned[j * rows : (j + 1) * rows]
    for i in range(near):
        x_scaled(i).start()
    for off in range(1, nodes):
        swap_turned(off).start()
        swap_scaled(off).start()
    lax.fori_loop(1, chunks, lambda c, carry: (x_hidden(c).start(), carry)[1], 0)
    for off in range(1, nodes):
        swap_turned(off).wait_recv()

    def make_lone(d, carry):
        part = sall[d].reshape(4 * rows, slots)
        units = hid[:slots, columns(chunks)]
        product = jnp.dot(part, units, preferred_element_type=F32).astype(BF16)
        qacc[0, d] = product.reshape(2, 2 * rows, WIDE)
        scat[d, :, :, :slots] = sall[d, :, mx]
        return carry

    lax.fori_loop(0, depth, make_lone, 0)
    each_d(lambda d, k: y_copy(lone, 0, d).start())
    y_copy(lone, 0, mz).start()
    for off in range(1, nodes):
        swap_scaled(off).wait_recv()

    def make_hidden(c):
        slot = c % 2
        w_copy(c, slot).wait()

        @pl.when(c + 1 < total_chunks)
        def _():
            w_copy(c + 1, 1 - slot).start()

        total = jnp.dot(g[0], wbuf[slot, :half, :], preferred_element_type=F32)
        for i in range(1, nodes):
            total += jnp.dot(
                g[i], wbuf[slot, i * half : (i + 1) * half, :], preferred_element_type=F32
            )
        gh_ref[:, columns(c)] = total.astype(BF16)

    def hidden_range(start, stop):
        lax.fori_loop(start, stop, lambda c, carry: (make_hidden(c), carry)[1], 0)

    def send(c, d):
        k = jnp.abs(d - mz)

        @pl.when((k > 1) | ((k == 1) & jnp.logical_not(late(c))))
        def _():
            y_copy(main, c, d).start()

    def make_first(owner, i):
        d = owner * near + nth(owner, i)
        part = scat[d].reshape(2 * rows, 2 * slots)
        product = jnp.dot(part, hid[:, :WIDE], preferred_element_type=F32).astype(BF16)
        acc[0, d] = product.reshape(2, rows, WIDE)
        send(0, d)

    def single(f, c, d, rising):
        inside = not_first if rising else not_last
        into = f.up if rising else f.dn
        y_copy(f, c, d).wait_recv()

        @pl.when(inside)
        def _():
            z_copy(f, c, d, rising, False).wait_recv()
            f.acc[c, d, my] = added(f.acc[c, d, my], f.ry[c, d], into[c, d, my])

        @pl.when(jnp.logical_not(inside))
        def _():
            f.acc[c, d, my] = added(f.acc[c, d, my], f.ry[c, d])

        z_copy(f, c, d, rising, False).start()

    def pass_on(f, c, rising, first=None, least=2):
        for k in range(first or last, least - 1, -1):
            d = mz + k if rising else mz - k

            @pl.when((d <= last) if rising else (d >= 0))
            def _():
                single(f, c, d, rising)

    def hand_over(f, c, rising):
        inside = not_first if rising else not_last
        into = f.up if rising else f.dn
        d = mz + 1 if rising else mz - 1

        @pl.when(f.late(c))
        def _():
            @pl.when(inside)
            def _():
                z_copy(f, c, d, rising, False).wait_recv()
                f.acc[c, d, my] = added(f.acc[c, d, my], into[c, d, my])

            z_copy(f, c, d, rising, True).start()

        @pl.when(jnp.logical_not(f.late(c)))
        def _():
            single(f, c, d, rising)

    def at_ends(run):
        @pl.when(mz == 0)
        def _():
            run(True)

        @pl.when(mz == last)
        def _():
            run(False)

    done = 0

    def hidden_until(share):
        nonlocal done
        until = total_chunks * share // 14
        hidden_range(done, until)
        done = until

    hidden_until(5)
    at_ends(lambda rising: pass_on(lone, 0, rising, last, last))
    hidden_until(7)
    at_ends(lambda rising: pass_on(lone, 0, rising, last - 1, 2))
    for i in range(near):
        if i == 1:
            hidden_until(9)
            at_ends(lambda rising: hand_over(lone, 0, rising))
        x_scaled(i).wait_recv()
        for off in range(1, nodes):
            forward(off, i).start()
        if i == 0:
            x_hidden(0).wait_recv()
        make_first(node, i)
        for off in range(1, nodes):
            forward(off, i).wait_recv()
            make_first((node + nodes - off) % nodes, i)
    if near == 1:
        at_ends(lambda rising: hand_over(lone, 0, rising))

    def make(c):
        x_hidden(c).wait_recv()
        units = hid[:, columns(c)]

        def two(j, carry):
            part = scat[pl.ds(2 * j, 2)].reshape(4 * rows, 2 * slots)
            product = jnp.dot(part, units, preferred_element_type=F32).astype(BF16)
            acc[c, pl.ds(2 * j, 2)] = product.reshape(2, 2, rows, WIDE)
            return carry

        lax.fori_loop(0, depth // 2, two, 0)

        each_d(lambda d, k: send(c, d))

    def settle(c):
        @pl.when(late(c))
        def _():
            @pl.when(not_first)
            def _():
                z_copy(main, c, mz, True, True).wait_recv()
                acc[c, mz] = added(acc[c, mz], up[c, mz])

            @pl.when(not_last)
            def _():
                z_copy(main, c, mz, False, True).wait_recv()
                acc[c, mz] = added(acc[c, mz], dn[c, mz])

            y_copy(main, c, mz).start()

    def finish(c):
        y_copy(main, c, mz).wait_recv()
        cols = columns(c)

        @pl.when(late(c))
        def _():
            gw_ref[:, cols] = added(acc[c, mz, my], ry[c, mz])

        @pl.when(jnp.logical_not(late(c)))
        def _():
            @pl.when(not_first)
            def _():
                z_copy(main, c, mz, True, False).wait_recv()

            @pl.when(not_last)
            def _():
                z_copy(main, c, mz, False, False).wait_recv()

            @pl.when(mz == 0)
            def _():
                gw_ref[:, cols] = added(acc[c, mz, my], ry[c, mz], dn[c, mz, my])

            @pl.when(mz == last)
            def _():
                gw_ref[:, cols] = added(acc[c, mz, my], ry[c, mz], up[c, mz, my])

            @pl.when(not_first & not_last)
            def _():
                gw_ref[:, cols] = added(
                    acc[c, mz, my], ry[c, mz], up[c, mz, my], dn[c, mz, my]
                )

    def within(c, run):
        @pl.when((c >= 0) & (c < chunks))
        def _():
            run(c)

    def finish_lone():
        y_copy(lone, 0, mz).wait_recv()

        @pl.when(not_first)
        def _():
            z_copy(lone, 0, mz, True, False).wait_recv()

        @pl.when(not_last)
        def _():
            z_copy(lone, 0, mz, False, False).wait_recv()

        own_part, across = qacc[0, mz, my], qry[0, mz]

        @pl.when(mz == 0)
        def _():
            qacc[0, mz, my] = added(own_part, across, qdn[0, mz, my])

        @pl.when(mz == last)
        def _():
            qacc[0, mz, my] = added(own_part, across, qup[0, mz, my])

        @pl.when(not_first & not_last)
        def _():
            qacc[0, mz, my] = added(own_part, across, qup[0, mz, my], qdn[0, mz, my])

        x_lone().start()

    def x_lone():
        src = qacc.at[0, mz, my, pl.ds(pl.multiple_of(px * rows, rows), rows)]
        return remote(src, qrx, qxsend, qxrecv, to_x)

    settled = AHEAD + HOP * last + DEFER
    below, above = mz, last - mz

    def turn(dist):
        return dist - 1 + jnp.minimum(dist - 1, 1)

    finished = last + 3

    def step(t, carry):
        @pl.when((t > 0) & (t < chunks))
        def _():
            make(t)

        @pl.when((t >= NEAR) & (t < chunks + NEAR) & jnp.logical_not(late(t - NEAR)))
        def _():
            y_copy(main, t - NEAR, mz).start()

        rise = t - AHEAD - HOP * below
        fall = t - AHEAD - HOP * above

        @pl.when(not_last)
        def _():
            within(rise, lambda c: pass_on(main, c, True))

            @pl.when(not_first & (t == turn(below)))
            def _():
                pass_on(lone, 0, True, None, 1)

        @pl.when(not_first)
        def _():
            within(fall, lambda c: pass_on(main, c, False))

            @pl.when(not_last & (t == turn(above)))
            def _():
                pass_on(lone, 0, False, None, 1)

        @pl.when(t + done < total_chunks)
        def _():
            make_hidden(t + done)

        @pl.when(not_last)
        def _():
            within(rise - DEFER, lambda c: hand_over(main, c, True))

        @pl.when(not_first)
        def _():
            within(fall - DEFER, lambda c: hand_over(main, c, False))

        within(t - settled, settle)
        within(t - settled - LAST, finish)

        @pl.when(t == finished)
        def _():
            finish_lone()

        return carry

    steps = max(chunks + settled + LAST, total_chunks - done, finished + 1)
    lax.fori_loop(0, steps, step, 0)
    x_lone().wait_recv()
    mine = pl.ds(pl.multiple_of(mx * rows, rows), rows)
    gw_ref[:, columns(chunks)] = added(qacc[0, mz, my, mine], qrx[...])
    x_lone().wait_send()

    for off in range(1, nodes):
        swap_turned(off).wait_send()
        swap_scaled(off).wait_send()
        for i in range(near):
            forward(off, i).wait_send()
    for i in range(near):
        x_scaled(i).wait_send()

    def drain(f, c):
        y_copy(f, c, mz).wait_send()

        def one(d, k):
            if k > 1:
                y_copy(f, c, d).wait_send()
            else:
                @pl.when(jnp.logical_not(f.late(c)))
                def _():
                    y_copy(f, c, d).wait_send()

        each_d(one)
        for k in range(1, depth):
            for rising in (True, False):
                d = mz + k if rising else mz - k

                @pl.when((d <= last) if rising else (d >= 0))
                def _():
                    if k > 1:
                        z_copy(f, c, d, rising, False).wait_send()
                    else:
                        @pl.when(f.late(c))
                        def _():
                            z_copy(f, c, d, rising, True).wait_send()

                        @pl.when(jnp.logical_not(f.late(c)))
                        def _():
                            z_copy(f, c, d, rising, False).wait_send()

    def drain_main(c, carry):
        x_hidden(c).wait_send()
        drain(main, c)
        return carry

    lax.fori_loop(0, chunks, drain_main, 0)
    drain(lone, 0)


def body(grad_out, gate_prob, hidden, w_down, slot_counts):
    slots, half = grad_out.shape
    nodes, groups = lax.axis_size("node"), lax.axis_size("grp")
    depth = groups // 4
    near = depth // nodes
    model = w_down.shape[0]
    rows = model // groups
    units = hidden.shape[1]
    chunks = -(-units // WIDE)
    extra = chunks * WIDE - units
    if extra:
        hidden = jnp.pad(hidden, ((0, 0), (0, extra)))
        w_down = jnp.pad(w_down, ((0, 0), (0, extra)))
    dma = pltpu.SemaphoreType.DMA
    vmem = pl.BlockSpec(memory_space=pltpu.VMEM)
    smem = pl.BlockSpec(memory_space=pltpu.SMEM)
    anywhere = pl.BlockSpec(memory_space=pl.ANY)
    grad_hidden, grad_weight = pl.pallas_call(
        functools.partial(kernel, (nodes, depth, chunks)),
        out_shape=(
            pltpu.VMEM((slots, chunks * WIDE), BF16),
            pltpu.VMEM((rows, chunks * WIDE), BF16),
        ),
        in_specs=[anywhere, vmem, smem, anywhere, anywhere],
        out_specs=(vmem, vmem),
        scratch_shapes=[
            pltpu.VMEM((slots, half), BF16),
            pltpu.VMEM((nodes, slots, half), BF16),
            pltpu.VMEM((depth, 2, 2, rows, slots), BF16),
            pltpu.VMEM((depth, 2, rows, 2 * slots), BF16),
            pltpu.VMEM((2 * slots, chunks * WIDE), BF16),
            pltpu.VMEM((2, model, WIDE), BF16),
            pltpu.VMEM((chunks - 1, depth, 2, rows, WIDE), BF16),
            pltpu.VMEM((chunks - 1, depth, rows, WIDE), BF16),
            pltpu.VMEM((chunks - 1, depth, 2, rows, WIDE), BF16),
            pltpu.VMEM((chunks - 1, depth, 2, rows, WIDE), BF16),
            pltpu.VMEM((1, depth, 2, 2 * rows, WIDE), BF16),
            pltpu.VMEM((1, depth, 2 * rows, WIDE), BF16),
            pltpu.VMEM((1, depth, 2, 2 * rows, WIDE), BF16),
            pltpu.VMEM((1, depth, 2, 2 * rows, WIDE), BF16),
            pltpu.VMEM((rows, WIDE), BF16),
            dma(()),
            dma(()),
            dma((2,)),
            dma((nodes,)),
            dma((nodes,)),
            dma((nodes,)),
            dma((nodes,)),
            dma((near,)),
            dma((near,)),
            dma((nodes, near)),
            dma((nodes, near)),
            dma((chunks,)),
            dma((chunks,)),
            dma((chunks, depth)),
            dma((chunks, depth)),
            dma((chunks, depth)),
            dma((chunks, depth)),
            dma((chunks, depth)),
            dma((chunks, depth)),
        ]
        + [dma((1, depth))] * 6
        + [dma(())] * 2,
        compiler_params=pltpu.CompilerParams(
            collective_id=0, has_side_effects=True, vmem_limit_bytes=54 * 1024 * 1024
        ),
    )(grad_out, gate_prob, slot_counts, hidden, w_down)
    return grad_hidden[:, :units], grad_weight[:, :units]


def solution(mesh):
    return jax.shard_map(
        body,
        mesh=mesh,
        in_specs=(P("grp", "node"), P("grp"), P("grp", "node"), P(None, "node"), P("grp")),
        out_specs=(P("grp", "node"), P("grp", "node")),
        check_vma=False,
    )
```

```python
import functools
from types import SimpleNamespace

import jax
import jax.numpy as jnp
from jax import lax
from jax.experimental import pallas as pl
from jax.experimental.pallas import tpu as pltpu
from jax.sharding import PartitionSpec as P

MESH = pl.DeviceIdType.MESH
LANES = 128
WIDE = 2 * LANES
AHEAD = 1
HOP = 1
DEFER = 1
NEAR = 3
LAST = 3
SHARES = (3, 5, 7, 9)
F32, BF16 = jnp.float32, jnp.bfloat16


def added(*terms):
    total = terms[0].astype(F32)
    for term in terms[1:]:
        total += term.astype(F32)
    return total.astype(BF16)


def kernel(
    dims, go_any, gate_any, count_any, hid_any, w_ref, gh_ref, gw_ref,
    gate_ref, count_ref, go, g, sall, scat, hid, wbuf, acc, ry, up, dn, qacc, qry, qup, qdn, qrx,
    gosem, hsem, wsem, gsend, grecv, ssend, srecv, xsend, xrecv, fsend, frecv,
    hsend, hrecv, ysend, yrecv, usend, urecv, dsend, drecv,
    qysend, qyrecv, qusend, qurecv, qdsend, qdrecv, qxsend, qxrecv,
):
    nodes, depth, total_chunks = dims
    chunks = total_chunks - 1
    node = lax.axis_index("node")
    me = lax.axis_index("grp")
    mx, my, mz = me % 2, (me // 2) % 2, me // 4
    px, py = 1 - mx, 1 - my
    slots, half = go.shape
    rows = acc.shape[3]
    near = depth // nodes
    last = depth - 1
    not_first, not_last = mz > 0, mz < last

    to_x = {"grp": me + 1 - 2 * mx}
    to_y = {"grp": me + 2 - 4 * my}
    to_up, to_down = {"grp": me + 4}, {"grp": me - 4}

    def columns(c):
        return pl.ds(pl.multiple_of(c * WIDE, WIDE), WIDE)

    def w_copy(c, slot):
        return pltpu.make_async_copy(w_ref.at[:, columns(c)], wbuf.at[slot], wsem.at[slot])

    own = pl.ds(0, slots)
    theirs = pl.ds(slots, slots)
    first, rest, final = pl.ds(0, WIDE), pl.ds(WIDE, (chunks - 1) * WIDE), columns(chunks)

    def take(cols, i):
        return pltpu.make_async_copy(hid_any.at[:, cols], hid.at[own, cols], hsem.at[i])

    take_grad = pltpu.make_async_copy(go_any, go, gosem.at[0])
    take_gate = pltpu.make_async_copy(gate_any, gate_ref, gosem.at[1])
    take_count = pltpu.make_async_copy(count_any, count_ref, gosem.at[2])
    take_count.start()
    take_gate.start()
    take_grad.start()
    take(first, 0).start()
    take(final, 1).start()

    barrier = pltpu.get_barrier_semaphore()

    def greet(target):
        pl.semaphore_signal(barrier, inc=1, device_id=target, device_id_type=MESH)

    greet(to_x)
    greet(to_y)
    for off in range(1, nodes):
        greet({"node": (node + off) % nodes})

    @pl.when(not_first)
    def _():
        greet(to_down)

    @pl.when(not_last)
    def _():
        greet(to_up)

    def remote(src, dst, ssem, rsem, target):
        return pltpu.make_async_remote_copy(
            src_ref=src, dst_ref=dst, send_sem=ssem, recv_sem=rsem,
            device_id=target, device_id_type=MESH,
        )

    def peer(off):
        return {"node": (node + off) % nodes}

    def swap_scaled(off):
        return remote(g.at[node], g.at[node], gsend.at[off], grecv.at[off], peer(off))

    def swap_turned(off):
        ref = sall.at[pl.ds(node * near, near)]
        return remote(ref, ref, ssend.at[off], srecv.at[off], peer(off))

    def nth(owner, i):
        return jnp.where(2 * owner < nodes, i, near - 1 - i)

    def x_scaled(i):
        d = node * near + nth(node, i)
        dst = scat.at[d, :, :, theirs]
        return remote(sall.at[d, :, px], dst, xsend.at[i], xrecv.at[i], to_x)

    def forward(off, i):
        ref = scat.at[node * near + nth(node, i), :, :, theirs]
        return remote(ref, ref, fsend.at[off, i], frecv.at[off, i], peer(off))

    def x_hidden(c):
        return remote(
            hid.at[own, columns(c)], hid.at[theirs, columns(c)],
            hsend.at[c], hrecv.at[c], to_x,
        )

    def late(c):
        return (c % 2 == 1) & (c > 2) & (c < chunks - 3)

    main = SimpleNamespace(
        acc=acc, ry=ry, up=up, dn=dn, late=late, ysend=ysend, yrecv=yrecv,
        usend=usend, urecv=urecv, dsend=dsend, drecv=drecv,
    )
    lone = SimpleNamespace(
        acc=qacc, ry=qry, up=qup, dn=qdn, late=lambda c: c < 0, ysend=qysend, yrecv=qyrecv,
        usend=qusend, urecv=qurecv, dsend=qdsend, drecv=qdrecv,
    )

    def y_copy(f, c, d):
        return remote(
            f.acc.at[c, d, py], f.ry.at[c, d], f.ysend.at[c, d], f.yrecv.at[c, d], to_y
        )

    def z_copy(f, c, d, rising, both):
        if both:
            pick = lambda ref: ref.at[c, d]
        else:
            pick = lambda ref: ref.at[c, d, my]
        if rising:
            return remote(
                pick(f.acc), pick(f.up), f.usend.at[c, d], f.urecv.at[c, d], to_up
            )
        return remote(
            pick(f.acc), pick(f.dn), f.dsend.at[c, d], f.drecv.at[c, d], to_down
        )

    def each_d(run, least=1):
        for k in range(last, least - 1, -1):
            @pl.when(mz + k <= last)
            def _():
                run(mz + k, k)

            @pl.when(mz - k >= 0)
            def _():
                run(mz - k, k)

    take_count.wait()
    take_gate.wait()
    take_grad.wait()
    take(rest, 2).start()
    w_copy(0, 0).start()

    live = lax.broadcasted_iota(jnp.int32, (LANES, slots), 1) < count_ref[0]
    gate = jnp.broadcast_to(gate_ref[...].reshape(1, slots), (LANES, slots))
    gate = jnp.where(live, gate, 0.0).T
    for i in range(half // LANES):
        cols = pl.ds(i * LANES, LANES)
        scaled = (go[:, cols].astype(F32) * gate).astype(BF16)
        g[node, :, cols] = scaled
        turned = scaled.T
        for j in range(LANES // rows):
            b = i * (LANES // rows) + j
            sall[node * near + b // 4, (b // 2) % 2, b % 2] = turned[j * rows : (j + 1) * rows]
    pl.semaphore_wait(
        barrier, 1 + nodes + not_first.astype(jnp.int32) + not_last.astype(jnp.int32)
    )
    take(first, 0).wait()
    x_hidden(0).start()
    for i in range(near):
        x_scaled(i).start()
    for off in range(1, nodes):
        swap_turned(off).start()
    for off in range(1, nodes):
        swap_scaled(off).start()
    take(final, 1).wait()

    def lone_row(j):
        i = j % near
        i = jnp.where(2 * mz < depth, near - 1 - i, i)
        return (node + nodes - j // near) % nodes * near + i

    def make_lone(j, carry):
        d = lone_row(j)
        part = sall[d].reshape(4 * rows, slots)
        units = hid[:slots, columns(chunks)]
        product = jnp.dot(part, units, preferred_element_type=F32).astype(BF16)
        qacc[0, d] = product.reshape(2, 2 * rows, WIDE)

        @pl.when(d != mz)
        def _():
            y_copy(lone, 0, d).start()

        scat[d, :, :, :slots] = sall[d, :, mx]
        return carry

    def lone_rows(off):
        lax.fori_loop(off * near, off * near + near, make_lone, 0)

    lone_rows(0)
    take(rest, 2).wait()
    lax.fori_loop(1, chunks, lambda c, carry: (x_hidden(c).start(), carry)[1], 0)
    for off in range(1, nodes):
        swap_turned(off).wait_recv()
        lone_rows(off)
    y_copy(lone, 0, mz).start()
    for off in range(1, nodes):
        swap_scaled(off).wait_recv()

    def make_hidden(c):
        slot = c % 2
        w_copy(c, slot).wait()

        @pl.when(c + 1 < total_chunks)
        def _():
            w_copy(c + 1, 1 - slot).start()

        total = jnp.dot(g[0], wbuf[slot, :half, :], preferred_element_type=F32)
        for i in range(1, nodes):
            total += jnp.dot(
                g[i], wbuf[slot, i * half : (i + 1) * half, :], preferred_element_type=F32
            )
        gh_ref[:, columns(c)] = total.astype(BF16)

    def hidden_range(start, stop):
        lax.fori_loop(start, stop, lambda c, carry: (make_hidden(c), carry)[1], 0)

    def send(c, d):
        k = jnp.abs(d - mz)

        @pl.when((k > 1) | ((k == 1) & jnp.logical_not(late(c))))
        def _():
            y_copy(main, c, d).start()

    def make_first(owner, i):
        d = owner * near + nth(owner, i)
        part = scat[d].reshape(2 * rows, 2 * slots)
        product = jnp.dot(part, hid[:, :WIDE], preferred_element_type=F32).astype(BF16)
        acc[0, d] = product.reshape(2, rows, WIDE)
        send(0, d)

    def single(f, c, d, rising):
        inside = not_first if rising else not_last
        into = f.up if rising else f.dn
        y_copy(f, c, d).wait_recv()

        @pl.when(inside)
        def _():
            z_copy(f, c, d, rising, False).wait_recv()
            f.acc[c, d, my] = added(f.acc[c, d, my], f.ry[c, d], into[c, d, my])

        @pl.when(jnp.logical_not(inside))
        def _():
            f.acc[c, d, my] = added(f.acc[c, d, my], f.ry[c, d])

        z_copy(f, c, d, rising, False).start()

    def pass_on(f, c, rising, first=None, least=2):
        for k in range(first or last, least - 1, -1):
            d = mz + k if rising else mz - k

            @pl.when((d <= last) if rising else (d >= 0))
            def _():
                single(f, c, d, rising)

    def hand_over(f, c, rising):
        inside = not_first if rising else not_last
        into = f.up if rising else f.dn
        d = mz + 1 if rising else mz - 1

        @pl.when(f.late(c))
        def _():
            @pl.when(inside)
            def _():
                z_copy(f, c, d, rising, False).wait_recv()
                f.acc[c, d, my] = added(f.acc[c, d, my], into[c, d, my])

            z_copy(f, c, d, rising, True).start()

        @pl.when(jnp.logical_not(f.late(c)))
        def _():
            single(f, c, d, rising)

    def at_ends(run):
        @pl.when(mz == 0)
        def _():
            run(True)

        @pl.when(mz == last)
        def _():
            run(False)

    done = 0

    def hidden_until(share):
        nonlocal done
        until = total_chunks * share // 14
        hidden_range(done, until)
        done = until

    def lone_pass(start, stop):
        def one(j, carry):
            @pl.when(lone_row(j) != mz)
            def _():
                at_ends(lambda rising: single(lone, 0, lone_row(j), rising))

            return carry

        lax.fori_loop(start, stop, one, 0)

    hidden_until(SHARES[0])
    lone_pass(0, 1)
    hidden_until(SHARES[1])
    lone_pass(1, 2)
    hidden_until(SHARES[2])
    lone_pass(2, 3)
    for i in range(near):
        if i == near - 1:
            hidden_until(SHARES[3])
            lone_pass(3, depth)
        x_scaled(i).wait_recv()
        for off in range(1, nodes):
            forward(off, i).start()
        if i == 0:
            x_hidden(0).wait_recv()
        make_first(node, i)
        for off in range(1, nodes):
            forward(off, i).wait_recv()
            make_first((node + nodes - off) % nodes, i)
    def make(c):
        x_hidden(c).wait_recv()
        units = hid[:, columns(c)]

        def two(j, carry):
            part = scat[pl.ds(2 * j, 2)].reshape(4 * rows, 2 * slots)
            product = jnp.dot(part, units, preferred_element_type=F32).astype(BF16)
            acc[c, pl.ds(2 * j, 2)] = product.reshape(2, 2, rows, WIDE)
            return carry

        lax.fori_loop(0, depth // 2, two, 0)

        each_d(lambda d, k: send(c, d))

    def settle(c):
        @pl.when(late(c))
        def _():
            @pl.when(not_first)
            def _():
                z_copy(main, c, mz, True, True).wait_recv()
                acc[c, mz] = added(acc[c, mz], up[c, mz])

            @pl.when(not_last)
            def _():
                z_copy(main, c, mz, False, True).wait_recv()
                acc[c, mz] = added(acc[c, mz], dn[c, mz])

            y_copy(main, c, mz).start()

    def finish(c):
        y_copy(main, c, mz).wait_recv()
        cols = columns(c)

        @pl.when(late(c))
        def _():
            gw_ref[:, cols] = added(acc[c, mz, my], ry[c, mz])

        @pl.when(jnp.logical_not(late(c)))
        def _():
            @pl.when(not_first)
            def _():
                z_copy(main, c, mz, True, False).wait_recv()

            @pl.when(not_last)
            def _():
                z_copy(main, c, mz, False, False).wait_recv()

            @pl.when(mz == 0)
            def _():
                gw_ref[:, cols] = added(acc[c, mz, my], ry[c, mz], dn[c, mz, my])

            @pl.when(mz == last)
            def _():
                gw_ref[:, cols] = added(acc[c, mz, my], ry[c, mz], up[c, mz, my])

            @pl.when(not_first & not_last)
            def _():
                gw_ref[:, cols] = added(
                    acc[c, mz, my], ry[c, mz], up[c, mz, my], dn[c, mz, my]
                )

    def within(c, run):
        @pl.when((c >= 0) & (c < chunks))
        def _():
            run(c)

    def finish_lone():
        y_copy(lone, 0, mz).wait_recv()

        @pl.when(not_first)
        def _():
            z_copy(lone, 0, mz, True, False).wait_recv()

        @pl.when(not_last)
        def _():
            z_copy(lone, 0, mz, False, False).wait_recv()

        own_part, across = qacc[0, mz, my], qry[0, mz]

        @pl.when(mz == 0)
        def _():
            qacc[0, mz, my] = added(own_part, across, qdn[0, mz, my])

        @pl.when(mz == last)
        def _():
            qacc[0, mz, my] = added(own_part, across, qup[0, mz, my])

        @pl.when(not_first & not_last)
        def _():
            qacc[0, mz, my] = added(own_part, across, qup[0, mz, my], qdn[0, mz, my])

        x_lone().start()

    def x_lone():
        src = qacc.at[0, mz, my, pl.ds(pl.multiple_of(px * rows, rows), rows)]
        return remote(src, qrx, qxsend, qxrecv, to_x)

    def drain(f, c):
        y_copy(f, c, mz).wait_send()

        def one(d, k):
            if k > 1:
                y_copy(f, c, d).wait_send()
            else:
                @pl.when(jnp.logical_not(f.late(c)))
                def _():
                    y_copy(f, c, d).wait_send()

        each_d(one)
        for k in range(1, depth):
            for rising in (True, False):
                d = mz + k if rising else mz - k

                @pl.when((d <= last) if rising else (d >= 0))
                def _():
                    if k > 1:
                        z_copy(f, c, d, rising, False).wait_send()
                    else:
                        @pl.when(f.late(c))
                        def _():
                            z_copy(f, c, d, rising, True).wait_send()

                        @pl.when(jnp.logical_not(f.late(c)))
                        def _():
                            z_copy(f, c, d, rising, False).wait_send()

    settled = AHEAD + HOP * last + DEFER
    below, above = mz, last - mz

    def turn(dist):
        return dist - 1 + jnp.minimum(dist - 1, 1)

    finished = last + 3

    def step(t, carry):
        @pl.when((t > 0) & (t < chunks))
        def _():
            make(t)

        @pl.when((t >= NEAR) & (t < chunks + NEAR) & jnp.logical_not(late(t - NEAR)))
        def _():
            y_copy(main, t - NEAR, mz).start()

        rise = t - AHEAD - HOP * below
        fall = t - AHEAD - HOP * above

        @pl.when(not_last)
        def _():
            within(rise, lambda c: pass_on(main, c, True))

            @pl.when(not_first & (t == turn(below)))
            def _():
                pass_on(lone, 0, True, None, 1)

        @pl.when(not_first)
        def _():
            within(fall, lambda c: pass_on(main, c, False))

            @pl.when(not_last & (t == turn(above)))
            def _():
                pass_on(lone, 0, False, None, 1)

        @pl.when(t + done < total_chunks)
        def _():
            make_hidden(t + done)

        @pl.when(not_last)
        def _():
            within(rise - DEFER, lambda c: hand_over(main, c, True))

        @pl.when(not_first)
        def _():
            within(fall - DEFER, lambda c: hand_over(main, c, False))

        within(t - settled, settle)
        def close(c):
            finish(c)
            x_hidden(c).wait_send()
            drain(main, c)

        within(t - settled - LAST, close)

        @pl.when(t == finished)
        def _():
            finish_lone()
            drain(lone, 0)

        return carry

    steps = max(chunks + settled + LAST, total_chunks - done, finished + 1)
    lax.fori_loop(0, steps, step, 0)
    x_lone().wait_recv()
    mine = pl.ds(pl.multiple_of(mx * rows, rows), rows)
    gw_ref[:, columns(chunks)] = added(qacc[0, mz, my, mine], qrx[...])
    x_lone().wait_send()

    for off in range(1, nodes):
        swap_turned(off).wait_send()
        swap_scaled(off).wait_send()
        for i in range(near):
            forward(off, i).wait_send()
    for i in range(near):
        x_scaled(i).wait_send()

def body(grad_out, gate_prob, hidden, w_down, slot_counts):
    slots, half = grad_out.shape
    nodes, groups = lax.axis_size("node"), lax.axis_size("grp")
    depth = groups // 4
    near = depth // nodes
    model = w_down.shape[0]
    rows = model // groups
    units = hidden.shape[1]
    chunks = -(-units // WIDE)
    extra = chunks * WIDE - units
    if extra:
        hidden = jnp.pad(hidden, ((0, 0), (0, extra)))
        w_down = jnp.pad(w_down, ((0, 0), (0, extra)))
    dma = pltpu.SemaphoreType.DMA
    vmem = pl.BlockSpec(memory_space=pltpu.VMEM)
    anywhere = pl.BlockSpec(memory_space=pl.ANY)
    hbm = pl.BlockSpec(memory_space=pltpu.HBM)
    grad_hidden, grad_weight = pl.pallas_call(
        functools.partial(kernel, (nodes, depth, chunks)),
        out_shape=(
            pltpu.VMEM((slots, chunks * WIDE), BF16),
            pltpu.VMEM((rows, chunks * WIDE), BF16),
        ),
        in_specs=[anywhere, anywhere, hbm, anywhere, anywhere],
        out_specs=(vmem, vmem),
        scratch_shapes=[
            pltpu.VMEM((slots,), F32),
            pltpu.SMEM((1,), jnp.int32),
            pltpu.VMEM((slots, half), BF16),
            pltpu.VMEM((nodes, slots, half), BF16),
            pltpu.VMEM((depth, 2, 2, rows, slots), BF16),
            pltpu.VMEM((depth, 2, rows, 2 * slots), BF16),
            pltpu.VMEM((2 * slots, chunks * WIDE), BF16),
            pltpu.VMEM((2, model, WIDE), BF16),
            pltpu.VMEM((chunks - 1, depth, 2, rows, WIDE), BF16),
            pltpu.VMEM((chunks - 1, depth, rows, WIDE), BF16),
            pltpu.VMEM((chunks - 1, depth, 2, rows, WIDE), BF16),
            pltpu.VMEM((chunks - 1, depth, 2, rows, WIDE), BF16),
            pltpu.VMEM((1, depth, 2, 2 * rows, WIDE), BF16),
            pltpu.VMEM((1, depth, 2 * rows, WIDE), BF16),
            pltpu.VMEM((1, depth, 2, 2 * rows, WIDE), BF16),
            pltpu.VMEM((1, depth, 2, 2 * rows, WIDE), BF16),
            pltpu.VMEM((rows, WIDE), BF16),
            dma((3,)),
            dma((3,)),
            dma((2,)),
            dma((nodes,)),
            dma((nodes,)),
            dma((nodes,)),
            dma((nodes,)),
            dma((near,)),
            dma((near,)),
            dma((nodes, near)),
            dma((nodes, near)),
            dma((chunks,)),
            dma((chunks,)),
            dma((chunks, depth)),
            dma((chunks, depth)),
            dma((chunks, depth)),
            dma((chunks, depth)),
            dma((chunks, depth)),
            dma((chunks, depth)),
        ]
        + [dma((1, depth))] * 6
        + [dma(())] * 2,
        compiler_params=pltpu.CompilerParams(
            collective_id=0, has_side_effects=True, vmem_limit_bytes=54 * 1024 * 1024
        ),
    )(grad_out, gate_prob, slot_counts, hidden, w_down)
    return grad_hidden[:, :units], grad_weight[:, :units]


def solution(mesh):
    return jax.shard_map(
        body,
        mesh=mesh,
        in_specs=(P("grp", "node"), P("grp"), P("grp", "node"), P(None, "node"), P("grp")),
        out_specs=(P("grp", "node"), P("grp", "node")),
        check_vma=False,
    )
```

```python
import functools
from types import SimpleNamespace

import jax
import jax.numpy as jnp
from jax import lax
from jax.experimental import pallas as pl
from jax.experimental.pallas import tpu as pltpu
from jax.sharding import PartitionSpec as P

MESH = pl.DeviceIdType.MESH
LANES = 128
WIDE = 2 * LANES
AHEAD = 1
HOP = 1
DEFER = 1
NEAR = 3
LAST = 3
SHARES = (3, 5, 8, 10)
F32, BF16 = jnp.float32, jnp.bfloat16


def added(*terms):
    total = terms[0].astype(F32)
    for term in terms[1:]:
        total += term.astype(F32)
    return total.astype(BF16)


def kernel(
    dims, go_any, gate_any, count_any, hid_any, w_ref, gh_ref, gw_ref,
    gate_ref, count_ref, go, g, sall, scat, hid, wbuf, acc, ry, up, dn, qacc, qry, qup, qdn, qrx,
    gosem, hsem, wsem, gsend, grecv, ssend, srecv, xsend, xrecv, fsend, frecv,
    hsend, hrecv, ysend, yrecv, usend, urecv, dsend, drecv,
    qysend, qyrecv, qusend, qurecv, qdsend, qdrecv, qxsend, qxrecv,
):
    nodes, depth, total_chunks = dims
    chunks = total_chunks - 1
    node = lax.axis_index("node")
    me = lax.axis_index("grp")
    mx, my, mz = me % 2, (me // 2) % 2, me // 4
    px, py = 1 - mx, 1 - my
    slots, half = go.shape
    rows = acc.shape[3]
    near = depth // nodes
    last = depth - 1
    not_first, not_last = mz > 0, mz < last

    to_x = {"grp": me + 1 - 2 * mx}
    to_y = {"grp": me + 2 - 4 * my}
    to_up, to_down = {"grp": me + 4}, {"grp": me - 4}

    def columns(c):
        return pl.ds(pl.multiple_of(c * WIDE, WIDE), WIDE)

    def w_copy(c, slot):
        return pltpu.make_async_copy(w_ref.at[:, columns(c)], wbuf.at[slot], wsem.at[slot])

    own = pl.ds(0, slots)
    theirs = pl.ds(slots, slots)
    first, rest, final = pl.ds(0, WIDE), pl.ds(WIDE, (chunks - 1) * WIDE), columns(chunks)

    def take(cols, i):
        return pltpu.make_async_copy(hid_any.at[:, cols], hid.at[own, cols], hsem.at[i])

    take_grad = pltpu.make_async_copy(go_any, go, gosem.at[0])
    take_gate = pltpu.make_async_copy(gate_any, gate_ref, gosem.at[1])
    take_count = pltpu.make_async_copy(count_any, count_ref, gosem.at[2])
    take_count.start()
    take_gate.start()
    take_grad.start()
    take(first, 0).start()
    take(final, 1).start()

    barrier = pltpu.get_barrier_semaphore()

    def greet(target):
        pl.semaphore_signal(barrier, inc=1, device_id=target, device_id_type=MESH)

    greet(to_x)
    greet(to_y)
    for off in range(1, nodes):
        greet({"node": (node + off) % nodes})

    @pl.when(not_first)
    def _():
        greet(to_down)

    @pl.when(not_last)
    def _():
        greet(to_up)

    def remote(src, dst, ssem, rsem, target):
        return pltpu.make_async_remote_copy(
            src_ref=src, dst_ref=dst, send_sem=ssem, recv_sem=rsem,
            device_id=target, device_id_type=MESH,
        )

    def peer(off):
        return {"node": (node + off) % nodes}

    def swap_scaled(off):
        return remote(g.at[node], g.at[node], gsend.at[off], grecv.at[off], peer(off))

    def swap_turned(off):
        ref = sall.at[pl.ds(node * near, near)]
        return remote(ref, ref, ssend.at[off], srecv.at[off], peer(off))

    def nth(owner, i):
        return jnp.where(2 * mz < depth, near - 1 - i, i)

    def x_scaled(i):
        d = node * near + nth(node, i)
        dst = scat.at[d, :, :, theirs]
        return remote(sall.at[d, :, px], dst, xsend.at[i], xrecv.at[i], to_x)

    def forward(off, i):
        ref = scat.at[node * near + nth(node, i), :, :, theirs]
        return remote(ref, ref, fsend.at[off, i], frecv.at[off, i], peer(off))

    def x_hidden(c):
        return remote(
            hid.at[own, columns(c)], hid.at[theirs, columns(c)],
            hsend.at[c], hrecv.at[c], to_x,
        )

    def late(c):
        return (c % 2 == 1) & (c > 2) & (c < chunks - 3)

    main = SimpleNamespace(
        acc=acc, ry=ry, up=up, dn=dn, late=late, ysend=ysend, yrecv=yrecv,
        usend=usend, urecv=urecv, dsend=dsend, drecv=drecv,
    )
    lone = SimpleNamespace(
        acc=qacc, ry=qry, up=qup, dn=qdn, late=lambda c: c < 0, ysend=qysend, yrecv=qyrecv,
        usend=qusend, urecv=qurecv, dsend=qdsend, drecv=qdrecv,
    )

    def y_copy(f, c, d):
        return remote(
            f.acc.at[c, d, py], f.ry.at[c, d], f.ysend.at[c, d], f.yrecv.at[c, d], to_y
        )

    def z_copy(f, c, d, rising, both):
        if both:
            pick = lambda ref: ref.at[c, d]
        else:
            pick = lambda ref: ref.at[c, d, my]
        if rising:
            return remote(
                pick(f.acc), pick(f.up), f.usend.at[c, d], f.urecv.at[c, d], to_up
            )
        return remote(
            pick(f.acc), pick(f.dn), f.dsend.at[c, d], f.drecv.at[c, d], to_down
        )

    def each_d(run, least=1):
        for k in range(last, least - 1, -1):
            @pl.when(mz + k <= last)
            def _():
                run(mz + k, k)

            @pl.when(mz - k >= 0)
            def _():
                run(mz - k, k)

    take_count.wait()
    take_gate.wait()
    take_grad.wait()
    take(rest, 2).start()
    w_copy(0, 0).start()

    live = lax.broadcasted_iota(jnp.int32, (LANES, slots), 1) < count_ref[0]
    gate = jnp.broadcast_to(gate_ref[...].reshape(1, slots), (LANES, slots))
    gate = jnp.where(live, gate, 0.0).T
    for i in range(half // LANES):
        cols = pl.ds(i * LANES, LANES)
        scaled = (go[:, cols].astype(F32) * gate).astype(BF16)
        g[node, :, cols] = scaled
        turned = scaled.T
        for j in range(LANES // rows):
            b = i * (LANES // rows) + j
            sall[node * near + b // 4, (b // 2) % 2, b % 2] = turned[j * rows : (j + 1) * rows]
    pl.semaphore_wait(
        barrier, 1 + nodes + not_first.astype(jnp.int32) + not_last.astype(jnp.int32)
    )
    take(first, 0).wait()
    x_hidden(0).start()
    for i in range(near):
        x_scaled(i).start()
    for off in range(1, nodes):
        swap_turned(off).start()
    for off in range(1, nodes):
        swap_scaled(off).start()
    take(final, 1).wait()

    def lone_row(j):
        i = j % near
        i = jnp.where(2 * mz < depth, near - 1 - i, i)
        return (node + nodes - j // near) % nodes * near + i

    def make_lone(j, carry):
        d = lone_row(j)
        part = sall[d].reshape(4 * rows, slots)
        units = hid[:slots, columns(chunks)]
        product = jnp.dot(part, units, preferred_element_type=F32).astype(BF16)
        qacc[0, d] = product.reshape(2, 2 * rows, WIDE)

        @pl.when(d != mz)
        def _():
            y_copy(lone, 0, d).start()

        scat[d, :, :, :slots] = sall[d, :, mx]
        return carry

    def lone_rows(off):
        lax.fori_loop(off * near, off * near + near, make_lone, 0)

    lone_rows(0)
    take(rest, 2).wait()
    lax.fori_loop(1, chunks, lambda c, carry: (x_hidden(c).start(), carry)[1], 0)
    for off in range(1, nodes):
        swap_turned(off).wait_recv()
        lone_rows(off)
    y_copy(lone, 0, mz).start()
    for off in range(1, nodes):
        swap_scaled(off).wait_recv()

    def make_hidden(c):
        slot = c % 2
        w_copy(c, slot).wait()

        @pl.when(c + 1 < total_chunks)
        def _():
            w_copy(c + 1, 1 - slot).start()

        total = jnp.dot(g[0], wbuf[slot, :half, :], preferred_element_type=F32)
        for i in range(1, nodes):
            total += jnp.dot(
                g[i], wbuf[slot, i * half : (i + 1) * half, :], preferred_element_type=F32
            )
        gh_ref[:, columns(c)] = total.astype(BF16)

    def hidden_range(start, stop):
        lax.fori_loop(start, stop, lambda c, carry: (make_hidden(c), carry)[1], 0)

    def send(c, d):
        k = jnp.abs(d - mz)

        @pl.when((k > 1) | ((k == 1) & jnp.logical_not(late(c))))
        def _():
            y_copy(main, c, d).start()

    def make_first(owner, i):
        d = owner * near + nth(owner, i)
        part = scat[d].reshape(2 * rows, 2 * slots)
        product = jnp.dot(part, hid[:, :WIDE], preferred_element_type=F32).astype(BF16)
        acc[0, d] = product.reshape(2, rows, WIDE)
        send(0, d)

    def single(f, c, d, rising):
        inside = not_first if rising else not_last
        into = f.up if rising else f.dn
        y_copy(f, c, d).wait_recv()

        @pl.when(inside)
        def _():
            z_copy(f, c, d, rising, False).wait_recv()
            f.acc[c, d, my] = added(f.acc[c, d, my], f.ry[c, d], into[c, d, my])

        @pl.when(jnp.logical_not(inside))
        def _():
            f.acc[c, d, my] = added(f.acc[c, d, my], f.ry[c, d])

        z_copy(f, c, d, rising, False).start()

    def pass_on(f, c, rising, first=None, least=2):
        for k in range(first or last, least - 1, -1):
            d = mz + k if rising else mz - k

            @pl.when((d <= last) if rising else (d >= 0))
            def _():
                single(f, c, d, rising)

    def hand_over(f, c, rising):
        inside = not_first if rising else not_last
        into = f.up if rising else f.dn
        d = mz + 1 if rising else mz - 1

        @pl.when(f.late(c))
        def _():
            @pl.when(inside)
            def _():
                z_copy(f, c, d, rising, False).wait_recv()
                f.acc[c, d, my] = added(f.acc[c, d, my], into[c, d, my])

            z_copy(f, c, d, rising, True).start()

        @pl.when(jnp.logical_not(f.late(c)))
        def _():
            single(f, c, d, rising)

    def at_ends(run):
        @pl.when(mz == 0)
        def _():
            run(True)

        @pl.when(mz == last)
        def _():
            run(False)

    done = 0

    def hidden_until(share):
        nonlocal done
        until = total_chunks * share // 14
        hidden_range(done, until)
        done = until

    def lone_pass(start, stop):
        def one(j, carry):
            @pl.when(lone_row(j) != mz)
            def _():
                at_ends(lambda rising: single(lone, 0, lone_row(j), rising))

            return carry

        lax.fori_loop(start, stop, one, 0)

    hidden_until(SHARES[0])
    lone_pass(0, 1)
    hidden_until(SHARES[1])
    lone_pass(1, 2)
    hidden_until(SHARES[2])
    lone_pass(2, 3)
    for i in range(near):
        if i == near - 1:
            hidden_until(SHARES[3])
            lone_pass(3, depth)
        x_scaled(i).wait_recv()
        for off in range(1, nodes):
            forward(off, i).start()
        if i == 0:
            x_hidden(0).wait_recv()
        make_first(node, i)
        for off in range(1, nodes):
            forward(off, i).wait_recv()
            make_first((node + nodes - off) % nodes, i)
    def make(c):
        x_hidden(c).wait_recv()
        units = hid[:, columns(c)]

        def two(j, carry):
            part = scat[pl.ds(2 * j, 2)].reshape(4 * rows, 2 * slots)
            product = jnp.dot(part, units, preferred_element_type=F32).astype(BF16)
            acc[c, pl.ds(2 * j, 2)] = product.reshape(2, 2, rows, WIDE)
            return carry

        lax.fori_loop(0, depth // 2, two, 0)

        each_d(lambda d, k: send(c, d))

    def settle(c):
        @pl.when(late(c))
        def _():
            @pl.when(not_first)
            def _():
                z_copy(main, c, mz, True, True).wait_recv()
                acc[c, mz] = added(acc[c, mz], up[c, mz])

            @pl.when(not_last)
            def _():
                z_copy(main, c, mz, False, True).wait_recv()
                acc[c, mz] = added(acc[c, mz], dn[c, mz])

            y_copy(main, c, mz).start()

    def finish(c):
        y_copy(main, c, mz).wait_recv()
        cols = columns(c)

        @pl.when(late(c))
        def _():
            gw_ref[:, cols] = added(acc[c, mz, my], ry[c, mz])

        @pl.when(jnp.logical_not(late(c)))
        def _():
            @pl.when(not_first)
            def _():
                z_copy(main, c, mz, True, False).wait_recv()

            @pl.when(not_last)
            def _():
                z_copy(main, c, mz, False, False).wait_recv()

            @pl.when(mz == 0)
            def _():
                gw_ref[:, cols] = added(acc[c, mz, my], ry[c, mz], dn[c, mz, my])

            @pl.when(mz == last)
            def _():
                gw_ref[:, cols] = added(acc[c, mz, my], ry[c, mz], up[c, mz, my])

            @pl.when(not_first & not_last)
            def _():
                gw_ref[:, cols] = added(
                    acc[c, mz, my], ry[c, mz], up[c, mz, my], dn[c, mz, my]
                )

    def within(c, run):
        @pl.when((c >= 0) & (c < chunks))
        def _():
            run(c)

    def finish_lone():
        y_copy(lone, 0, mz).wait_recv()

        @pl.when(not_first)
        def _():
            z_copy(lone, 0, mz, True, False).wait_recv()

        @pl.when(not_last)
        def _():
            z_copy(lone, 0, mz, False, False).wait_recv()

        own_part, across = qacc[0, mz, my], qry[0, mz]

        @pl.when(mz == 0)
        def _():
            qacc[0, mz, my] = added(own_part, across, qdn[0, mz, my])

        @pl.when(mz == last)
        def _():
            qacc[0, mz, my] = added(own_part, across, qup[0, mz, my])

        @pl.when(not_first & not_last)
        def _():
            qacc[0, mz, my] = added(own_part, across, qup[0, mz, my], qdn[0, mz, my])

        x_lone().start()

    def x_lone():
        src = qacc.at[0, mz, my, pl.ds(pl.multiple_of(px * rows, rows), rows)]
        return remote(src, qrx, qxsend, qxrecv, to_x)

    def drain(f, c):
        y_copy(f, c, mz).wait_send()

        def one(d, k):
            if k > 1:
                y_copy(f, c, d).wait_send()
            else:
                @pl.when(jnp.logical_not(f.late(c)))
                def _():
                    y_copy(f, c, d).wait_send()

        each_d(one)
        for k in range(1, depth):
            for rising in (True, False):
                d = mz + k if rising else mz - k

                @pl.when((d <= last) if rising else (d >= 0))
                def _():
                    if k > 1:
                        z_copy(f, c, d, rising, False).wait_send()
                    else:
                        @pl.when(f.late(c))
                        def _():
                            z_copy(f, c, d, rising, True).wait_send()

                        @pl.when(jnp.logical_not(f.late(c)))
                        def _():
                            z_copy(f, c, d, rising, False).wait_send()

    settled = AHEAD + HOP * last + DEFER
    below, above = mz, last - mz

    def turn(dist):
        return dist - 1 + jnp.minimum(dist - 1, 1)

    finished = last + 3

    def step(t, carry):
        @pl.when((t > 0) & (t < chunks))
        def _():
            make(t)

        @pl.when((t >= NEAR) & (t < chunks + NEAR) & jnp.logical_not(late(t - NEAR)))
        def _():
            y_copy(main, t - NEAR, mz).start()

        rise = t - AHEAD - HOP * below
        fall = t - AHEAD - HOP * above

        @pl.when(not_last)
        def _():
            within(rise, lambda c: pass_on(main, c, True))

            @pl.when(not_first & (t == turn(below)))
            def _():
                pass_on(lone, 0, True, None, 1)

        @pl.when(not_first)
        def _():
            within(fall, lambda c: pass_on(main, c, False))

            @pl.when(not_last & (t == turn(above)))
            def _():
                pass_on(lone, 0, False, None, 1)

        @pl.when(not_last)
        def _():
            within(rise - DEFER, lambda c: hand_over(main, c, True))

        @pl.when(not_first)
        def _():
            within(fall - DEFER, lambda c: hand_over(main, c, False))

        within(t - settled, settle)
        @pl.when(t + done < total_chunks)
        def _():
            make_hidden(t + done)

        def close(c):
            finish(c)
            x_hidden(c).wait_send()
            drain(main, c)

        within(t - settled - LAST, close)

        @pl.when(t == finished)
        def _():
            finish_lone()
            drain(lone, 0)

        return carry

    steps = max(chunks + settled + LAST, total_chunks - done, finished + 1)
    lax.fori_loop(0, steps, step, 0)
    x_lone().wait_recv()
    mine = pl.ds(pl.multiple_of(mx * rows, rows), rows)
    gw_ref[:, columns(chunks)] = added(qacc[0, mz, my, mine], qrx[...])
    x_lone().wait_send()

    for off in range(1, nodes):
        swap_turned(off).wait_send()
        swap_scaled(off).wait_send()
        for i in range(near):
            forward(off, i).wait_send()
    for i in range(near):
        x_scaled(i).wait_send()

def store(pieces, gh_ref, gw_ref, gh_any, gw_any, sems):
    slots, units = gh_any.shape
    rows, kept = slots // pieces, pl.ds(0, units)
    copies = [pltpu.make_async_copy(gw_ref.at[:, kept], gw_any, sems.at[pieces])]
    for i in range(pieces):
        part = pl.ds(i * rows, rows)
        copies.append(
            pltpu.make_async_copy(gh_ref.at[part, kept], gh_any.at[part], sems.at[i])
        )
    for copy in copies:
        copy.start()
    for copy in copies:
        copy.wait()


def body(grad_out, gate_prob, hidden, w_down, slot_counts):
    slots, half = grad_out.shape
    nodes, groups = lax.axis_size("node"), lax.axis_size("grp")
    depth = groups // 4
    near = depth // nodes
    model = w_down.shape[0]
    rows = model // groups
    units = hidden.shape[1]
    chunks = -(-units // WIDE)
    extra = chunks * WIDE - units
    if extra:
        hidden = jnp.pad(hidden, ((0, 0), (0, extra)))
        w_down = jnp.pad(w_down, ((0, 0), (0, extra)))
    dma = pltpu.SemaphoreType.DMA
    vmem = pl.BlockSpec(memory_space=pltpu.VMEM)
    anywhere = pl.BlockSpec(memory_space=pl.ANY)
    hbm = pl.BlockSpec(memory_space=pltpu.HBM)
    grad_hidden, grad_weight = pl.pallas_call(
        functools.partial(kernel, (nodes, depth, chunks)),
        out_shape=(
            pltpu.VMEM((slots, chunks * WIDE), BF16),
            pltpu.VMEM((rows, chunks * WIDE), BF16),
        ),
        in_specs=[anywhere, anywhere, hbm, anywhere, anywhere],
        out_specs=(vmem, vmem),
        scratch_shapes=[
            pltpu.VMEM((slots,), F32),
            pltpu.SMEM((1,), jnp.int32),
            pltpu.VMEM((slots, half), BF16),
            pltpu.VMEM((nodes, slots, half), BF16),
            pltpu.VMEM((depth, 2, 2, rows, slots), BF16),
            pltpu.VMEM((depth, 2, rows, 2 * slots), BF16),
            pltpu.VMEM((2 * slots, chunks * WIDE), BF16),
            pltpu.VMEM((2, model, WIDE), BF16),
            pltpu.VMEM((chunks - 1, depth, 2, rows, WIDE), BF16),
            pltpu.VMEM((chunks - 1, depth, rows, WIDE), BF16),
            pltpu.VMEM((chunks - 1, depth, 2, rows, WIDE), BF16),
            pltpu.VMEM((chunks - 1, depth, 2, rows, WIDE), BF16),
            pltpu.VMEM((1, depth, 2, 2 * rows, WIDE), BF16),
            pltpu.VMEM((1, depth, 2 * rows, WIDE), BF16),
            pltpu.VMEM((1, depth, 2, 2 * rows, WIDE), BF16),
            pltpu.VMEM((1, depth, 2, 2 * rows, WIDE), BF16),
            pltpu.VMEM((rows, WIDE), BF16),
            dma((3,)),
            dma((3,)),
            dma((2,)),
            dma((nodes,)),
            dma((nodes,)),
            dma((nodes,)),
            dma((nodes,)),
            dma((near,)),
            dma((near,)),
            dma((nodes, near)),
            dma((nodes, near)),
            dma((chunks,)),
            dma((chunks,)),
            dma((chunks, depth)),
            dma((chunks, depth)),
            dma((chunks, depth)),
            dma((chunks, depth)),
            dma((chunks, depth)),
            dma((chunks, depth)),
        ]
        + [dma((1, depth))] * 6
        + [dma(())] * 2,
        compiler_params=pltpu.CompilerParams(
            collective_id=0, has_side_effects=True, vmem_limit_bytes=54 * 1024 * 1024
        ),
    )(grad_out, gate_prob, slot_counts, hidden, w_down)
    return pl.pallas_call(
        functools.partial(store, 3),
        out_shape=(
            jax.ShapeDtypeStruct((slots, units), BF16),
            jax.ShapeDtypeStruct((rows, units), BF16),
        ),
        in_specs=[anywhere, anywhere],
        out_specs=(anywhere, anywhere),
        scratch_shapes=[dma((4,))],
        compiler_params=pltpu.CompilerParams(vmem_limit_bytes=8 * 1024 * 1024),
    )(grad_hidden, grad_weight)


def solution(mesh):
    return jax.shard_map(
        body,
        mesh=mesh,
        in_specs=(P("grp", "node"), P("grp"), P("grp", "node"), P(None, "node"), P("grp")),
        out_specs=(P("grp", "node"), P("grp", "node")),
        check_vma=False,
    )
```

```python
import functools
from types import SimpleNamespace

import jax
import jax.numpy as jnp
from jax import lax
from jax.experimental import pallas as pl
from jax.experimental.pallas import tpu as pltpu
from jax.sharding import PartitionSpec as P

MESH = pl.DeviceIdType.MESH
LANES = 128
WIDE = 2 * LANES
AHEAD = 1
HOP = 1
DEFER = 1
NEAR = 4
LAST = 3
SLOTS = 4
SHARES = (4, 8, 11, 14)
F32, BF16 = jnp.float32, jnp.bfloat16


def added(*terms):
    total = terms[0].astype(F32)
    for term in terms[1:]:
        total += term.astype(F32)
    return total.astype(BF16)


def kernel(
    dims, go_any, gate_any, count_any, hid_any, w_ref, gh_ref, gw_ref,
    gate_ref, count_ref, go, g, sall, scat, hid, wbuf, acc, ry, up, dn, qacc, qry, qup, qdn, qrx,
    gosem, hsem, wsem, gsend, grecv, ssend, srecv, xsend, xrecv, fsend, frecv,
    hsend, hrecv, ysend, yrecv, usend, urecv, dsend, drecv,
    qysend, qyrecv, qusend, qurecv, qdsend, qdrecv, qxsend, qxrecv,
):
    nodes, depth, total_chunks = dims
    chunks = total_chunks - 1
    node = lax.axis_index("node")
    me = lax.axis_index("grp")
    mx, my, mz = me % 2, (me // 2) % 2, me // 4
    px, py = 1 - mx, 1 - my
    slots, half = go.shape
    rows = acc.shape[3]
    near = depth // nodes
    last = depth - 1
    not_first, not_last = mz > 0, mz < last

    to_x = {"grp": me + 1 - 2 * mx}
    to_y = {"grp": me + 2 - 4 * my}
    to_up, to_down = {"grp": me + 4}, {"grp": me - 4}

    def columns(c):
        return pl.ds(pl.multiple_of(c * WIDE, WIDE), WIDE)

    def w_copy(c, slot):
        return pltpu.make_async_copy(w_ref.at[:, columns(c)], wbuf.at[slot], wsem.at[slot])

    own = pl.ds(0, slots)
    theirs = pl.ds(slots, slots)
    first, rest, final = pl.ds(0, WIDE), pl.ds(WIDE, (chunks - 1) * WIDE), columns(chunks)

    def take(cols, i):
        return pltpu.make_async_copy(hid_any.at[:, cols], hid.at[own, cols], hsem.at[i])

    take_grad = pltpu.make_async_copy(go_any, go, gosem.at[0])
    take_gate = pltpu.make_async_copy(gate_any, gate_ref, gosem.at[1])
    take_count = pltpu.make_async_copy(count_any, count_ref, gosem.at[2])
    take_count.start()
    take_gate.start()
    take_grad.start()
    take(first, 0).start()
    take(final, 1).start()

    barrier = pltpu.get_barrier_semaphore()

    def greet(target):
        pl.semaphore_signal(barrier, inc=1, device_id=target, device_id_type=MESH)

    greet(to_x)
    greet(to_y)
    for off in range(1, nodes):
        greet({"node": (node + off) % nodes})

    @pl.when(not_first)
    def _():
        greet(to_down)

    @pl.when(not_last)
    def _():
        greet(to_up)

    def remote(src, dst, ssem, rsem, target):
        return pltpu.make_async_remote_copy(
            src_ref=src, dst_ref=dst, send_sem=ssem, recv_sem=rsem,
            device_id=target, device_id_type=MESH,
        )

    def peer(off):
        return {"node": (node + off) % nodes}

    def swap_scaled(off):
        return remote(g.at[node], g.at[node], gsend.at[off], grecv.at[off], peer(off))

    def swap_turned(off):
        ref = sall.at[pl.ds(node * near, near)]
        return remote(ref, ref, ssend.at[off], srecv.at[off], peer(off))

    def nth(owner, i):
        return jnp.where(2 * mz < depth, near - 1 - i, i)

    def x_scaled(i):
        d = node * near + nth(node, i)
        dst = scat.at[d, :, :, theirs]
        return remote(sall.at[d, :, px], dst, xsend.at[i], xrecv.at[i], to_x)

    def forward(off, i):
        ref = scat.at[node * near + nth(node, i), :, :, theirs]
        return remote(ref, ref, fsend.at[off, i], frecv.at[off, i], peer(off))

    def x_hidden(c):
        return remote(
            hid.at[own, columns(c)], hid.at[theirs, columns(c)],
            hsend.at[c], hrecv.at[c], to_x,
        )

    def late(c):
        return (c % 2 == 1) & (c > 2) & (c < chunks - 3)

    main = SimpleNamespace(
        acc=acc, ry=ry, up=up, dn=dn, late=late, ysend=ysend, yrecv=yrecv,
        usend=usend, urecv=urecv, dsend=dsend, drecv=drecv,
    )
    lone = SimpleNamespace(
        acc=qacc, ry=qry, up=qup, dn=qdn, late=lambda c: c < 0, ysend=qysend, yrecv=qyrecv,
        usend=qusend, urecv=qurecv, dsend=qdsend, drecv=qdrecv,
    )

    def y_copy(f, c, d):
        return remote(
            f.acc.at[c, d, py], f.ry.at[c, d], f.ysend.at[c, d], f.yrecv.at[c, d], to_y
        )

    def z_copy(f, c, d, rising, both):
        if both:
            pick = lambda ref: ref.at[c, d]
        else:
            pick = lambda ref: ref.at[c, d, my]
        if rising:
            return remote(
                pick(f.acc), pick(f.up), f.usend.at[c, d], f.urecv.at[c, d], to_up
            )
        return remote(
            pick(f.acc), pick(f.dn), f.dsend.at[c, d], f.drecv.at[c, d], to_down
        )

    def each_d(run, least=1):
        for k in range(last, least - 1, -1):
            @pl.when(mz + k <= last)
            def _():
                run(mz + k, k)

            @pl.when(mz - k >= 0)
            def _():
                run(mz - k, k)

    take_count.wait()
    take_gate.wait()
    take_grad.wait()
    take(rest, 2).start()
    for c in range(min(SLOTS - 1, total_chunks)):
        w_copy(c, c).start()

    live = lax.broadcasted_iota(jnp.int32, (LANES, slots), 1) < count_ref[0]
    gate = jnp.broadcast_to(gate_ref[...].reshape(1, slots), (LANES, slots))
    gate = jnp.where(live, gate, 0.0).T
    for i in range(half // LANES):
        cols = pl.ds(i * LANES, LANES)
        scaled = (go[:, cols].astype(F32) * gate).astype(BF16)
        g[node, :, cols] = scaled
        turned = scaled.T
        for j in range(LANES // rows):
            b = i * (LANES // rows) + j
            sall[node * near + b // 4, (b // 2) % 2, b % 2] = turned[j * rows : (j + 1) * rows]
    pl.semaphore_wait(
        barrier, 1 + nodes + not_first.astype(jnp.int32) + not_last.astype(jnp.int32)
    )
    take(first, 0).wait()
    x_hidden(0).start()
    for i in range(near):
        x_scaled(i).start()
    for off in range(1, nodes):
        swap_turned(off).start()
    for off in range(1, nodes):
        swap_scaled(off).start()
    take(final, 1).wait()

    def lone_row(j):
        i = j % near
        i = jnp.where(2 * mz < depth, near - 1 - i, i)
        return (node + nodes - j // near) % nodes * near + i

    def make_lone(j, carry):
        d = lone_row(j)
        part = sall[d].reshape(4 * rows, slots)
        units = hid[:slots, columns(chunks)]
        product = jnp.dot(part, units, preferred_element_type=F32).astype(BF16)
        qacc[0, d] = product.reshape(2, 2 * rows, WIDE)

        @pl.when(d != mz)
        def _():
            y_copy(lone, 0, d).start()

        scat[d, :, :, :slots] = sall[d, :, mx]
        return carry

    def lone_rows(off):
        lax.fori_loop(off * near, off * near + near, make_lone, 0)

    lone_rows(0)
    take(rest, 2).wait()
    lax.fori_loop(1, chunks, lambda c, carry: (x_hidden(c).start(), carry)[1], 0)
    for off in range(1, nodes):
        swap_turned(off).wait_recv()
        lone_rows(off)
    y_copy(lone, 0, mz).start()
    for off in range(1, nodes):
        swap_scaled(off).wait_recv()

    def make_hidden(c):
        slot, ahead = c % SLOTS, c + SLOTS - 1
        w_copy(c, slot).wait()

        @pl.when(ahead < total_chunks)
        def _():
            w_copy(ahead, ahead % SLOTS).start()

        total = jnp.dot(g[0], wbuf[slot, :half, :], preferred_element_type=F32)
        for i in range(1, nodes):
            total += jnp.dot(
                g[i], wbuf[slot, i * half : (i + 1) * half, :], preferred_element_type=F32
            )
        gh_ref[:, columns(c)] = total.astype(BF16)

    def hidden_range(start, stop):
        lax.fori_loop(start, stop, lambda c, carry: (make_hidden(c), carry)[1], 0)

    def send(c, d):
        k = jnp.abs(d - mz)

        @pl.when((k > 1) | ((k == 1) & jnp.logical_not(late(c))))
        def _():
            y_copy(main, c, d).start()

    def make_first(owner, i):
        d = owner * near + nth(owner, i)
        part = scat[d].reshape(2 * rows, 2 * slots)
        product = jnp.dot(part, hid[:, :WIDE], preferred_element_type=F32).astype(BF16)
        acc[0, d] = product.reshape(2, rows, WIDE)
        send(0, d)

    def single(f, c, d, rising):
        inside = not_first if rising else not_last
        into = f.up if rising else f.dn
        y_copy(f, c, d).wait_recv()

        @pl.when(inside)
        def _():
            z_copy(f, c, d, rising, False).wait_recv()
            f.acc[c, d, my] = added(f.acc[c, d, my], f.ry[c, d], into[c, d, my])

        @pl.when(jnp.logical_not(inside))
        def _():
            f.acc[c, d, my] = added(f.acc[c, d, my], f.ry[c, d])

        z_copy(f, c, d, rising, False).start()

    def pass_on(f, c, rising, first=None, least=2):
        for k in range(first or last, least - 1, -1):
            d = mz + k if rising else mz - k

            @pl.when((d <= last) if rising else (d >= 0))
            def _():
                single(f, c, d, rising)

    def hand_over(f, c, rising):
        inside = not_first if rising else not_last
        into = f.up if rising else f.dn
        d = mz + 1 if rising else mz - 1

        @pl.when(f.late(c))
        def _():
            @pl.when(inside)
            def _():
                z_copy(f, c, d, rising, False).wait_recv()
                f.acc[c, d, my] = added(f.acc[c, d, my], into[c, d, my])

            z_copy(f, c, d, rising, True).start()

        @pl.when(jnp.logical_not(f.late(c)))
        def _():
            single(f, c, d, rising)

    def at_ends(run):
        @pl.when(mz == 0)
        def _():
            run(True)

        @pl.when(mz == last)
        def _():
            run(False)

    done = 0

    def hidden_until(share):
        nonlocal done
        until = total_chunks * share // 14
        hidden_range(done, until)
        done = until

    def lone_pass(start, stop):
        def one(j, carry):
            @pl.when(lone_row(j) != mz)
            def _():
                at_ends(lambda rising: single(lone, 0, lone_row(j), rising))

            return carry

        lax.fori_loop(start, stop, one, 0)

    hidden_until(SHARES[0])
    lone_pass(0, 1)
    hidden_until(SHARES[1])
    lone_pass(1, 2)
    hidden_until(SHARES[2])
    lone_pass(2, 3)
    for i in range(near):
        if i == near - 1:
            hidden_until(SHARES[3])
            lone_pass(3, depth)
        x_scaled(i).wait_recv()
        for off in range(1, nodes):
            forward(off, i).start()
        if i == 0:
            x_hidden(0).wait_recv()
        make_first(node, i)
        for off in range(1, nodes):
            forward(off, i).wait_recv()
            make_first((node + nodes - off) % nodes, i)
    def make(c):
        x_hidden(c).wait_recv()
        units = hid[:, columns(c)]

        def two(j, carry):
            part = scat[pl.ds(2 * j, 2)].reshape(4 * rows, 2 * slots)
            product = jnp.dot(part, units, preferred_element_type=F32).astype(BF16)
            acc[c, pl.ds(2 * j, 2)] = product.reshape(2, 2, rows, WIDE)
            return carry

        lax.fori_loop(0, depth // 2, two, 0)

        each_d(lambda d, k: send(c, d))

    def settle(c):
        @pl.when(late(c))
        def _():
            @pl.when(not_first)
            def _():
                z_copy(main, c, mz, True, True).wait_recv()
                acc[c, mz] = added(acc[c, mz], up[c, mz])

            @pl.when(not_last)
            def _():
                z_copy(main, c, mz, False, True).wait_recv()
                acc[c, mz] = added(acc[c, mz], dn[c, mz])

            y_copy(main, c, mz).start()

    def finish(c):
        y_copy(main, c, mz).wait_recv()
        cols = columns(c)

        @pl.when(late(c))
        def _():
            gw_ref[:, cols] = added(acc[c, mz, my], ry[c, mz])

        @pl.when(jnp.logical_not(late(c)))
        def _():
            @pl.when(not_first)
            def _():
                z_copy(main, c, mz, True, False).wait_recv()

            @pl.when(not_last)
            def _():
                z_copy(main, c, mz, False, False).wait_recv()

            @pl.when(mz == 0)
            def _():
                gw_ref[:, cols] = added(acc[c, mz, my], ry[c, mz], dn[c, mz, my])

            @pl.when(mz == last)
            def _():
                gw_ref[:, cols] = added(acc[c, mz, my], ry[c, mz], up[c, mz, my])

            @pl.when(not_first & not_last)
            def _():
                gw_ref[:, cols] = added(
                    acc[c, mz, my], ry[c, mz], up[c, mz, my], dn[c, mz, my]
                )

    def within(c, run):
        @pl.when((c >= 0) & (c < chunks))
        def _():
            run(c)

    def finish_lone():
        y_copy(lone, 0, mz).wait_recv()

        @pl.when(not_first)
        def _():
            z_copy(lone, 0, mz, True, False).wait_recv()

        @pl.when(not_last)
        def _():
            z_copy(lone, 0, mz, False, False).wait_recv()

        own_part, across = qacc[0, mz, my], qry[0, mz]

        @pl.when(mz == 0)
        def _():
            qacc[0, mz, my] = added(own_part, across, qdn[0, mz, my])

        @pl.when(mz == last)
        def _():
            qacc[0, mz, my] = added(own_part, across, qup[0, mz, my])

        @pl.when(not_first & not_last)
        def _():
            qacc[0, mz, my] = added(own_part, across, qup[0, mz, my], qdn[0, mz, my])

        x_lone().start()

    def x_lone():
        src = qacc.at[0, mz, my, pl.ds(pl.multiple_of(px * rows, rows), rows)]
        return remote(src, qrx, qxsend, qxrecv, to_x)

    def drain(f, c):
        y_copy(f, c, mz).wait_send()

        def one(d, k):
            if k > 1:
                y_copy(f, c, d).wait_send()
            else:
                @pl.when(jnp.logical_not(f.late(c)))
                def _():
                    y_copy(f, c, d).wait_send()

        each_d(one)
        for k in range(1, depth):
            for rising in (True, False):
                d = mz + k if rising else mz - k

                @pl.when((d <= last) if rising else (d >= 0))
                def _():
                    if k > 1:
                        z_copy(f, c, d, rising, False).wait_send()
                    else:
                        @pl.when(f.late(c))
                        def _():
                            z_copy(f, c, d, rising, True).wait_send()

                        @pl.when(jnp.logical_not(f.late(c)))
                        def _():
                            z_copy(f, c, d, rising, False).wait_send()

    settled = AHEAD + HOP * last + DEFER
    below, above = mz, last - mz

    def turn(dist):
        return dist - 1 + jnp.minimum(dist - 1, 1)

    finished = last + 3

    def step(t, carry):
        @pl.when((t > 0) & (t < chunks))
        def _():
            make(t)

        @pl.when((t >= NEAR) & (t < chunks + NEAR) & jnp.logical_not(late(t - NEAR)))
        def _():
            y_copy(main, t - NEAR, mz).start()

        rise = t - AHEAD - HOP * below
        fall = t - AHEAD - HOP * above

        @pl.when(not_last)
        def _():
            within(rise, lambda c: pass_on(main, c, True))

            @pl.when(not_first & (t == turn(below)))
            def _():
                pass_on(lone, 0, True, None, 1)

        @pl.when(not_first)
        def _():
            within(fall, lambda c: pass_on(main, c, False))

            @pl.when(not_last & (t == turn(above)))
            def _():
                pass_on(lone, 0, False, None, 1)

        @pl.when(not_last)
        def _():
            within(rise - DEFER, lambda c: hand_over(main, c, True))

        @pl.when(not_first)
        def _():
            within(fall - DEFER, lambda c: hand_over(main, c, False))

        within(t - settled, settle)
        @pl.when(t + done < total_chunks)
        def _():
            make_hidden(t + done)

        def close(c):
            finish(c)
            x_hidden(c).wait_send()
            drain(main, c)

        within(t - settled - LAST, close)

        @pl.when(t == finished)
        def _():
            finish_lone()
            drain(lone, 0)

        return carry

    steps = max(chunks + settled + LAST, total_chunks - done, finished + 1)
    lax.fori_loop(0, steps, step, 0)
    x_lone().wait_recv()
    mine = pl.ds(pl.multiple_of(mx * rows, rows), rows)
    gw_ref[:, columns(chunks)] = added(qacc[0, mz, my, mine], qrx[...])
    x_lone().wait_send()

    for off in range(1, nodes):
        swap_turned(off).wait_send()
        swap_scaled(off).wait_send()
        for i in range(near):
            forward(off, i).wait_send()
    for i in range(near):
        x_scaled(i).wait_send()

def store(pieces, gh_ref, gw_ref, gh_any, gw_any, sems):
    slots, units = gh_any.shape
    rows, kept = slots // pieces, pl.ds(0, units)
    copies = [pltpu.make_async_copy(gw_ref.at[:, kept], gw_any, sems.at[pieces])]
    for i in range(pieces):
        part = pl.ds(i * rows, rows)
        copies.append(
            pltpu.make_async_copy(gh_ref.at[part, kept], gh_any.at[part], sems.at[i])
        )
    for copy in copies:
        copy.start()
    for copy in copies:
        copy.wait()


def body(grad_out, gate_prob, hidden, w_down, slot_counts):
    slots, half = grad_out.shape
    nodes, groups = lax.axis_size("node"), lax.axis_size("grp")
    depth = groups // 4
    near = depth // nodes
    model = w_down.shape[0]
    rows = model // groups
    units = hidden.shape[1]
    chunks = -(-units // WIDE)
    extra = chunks * WIDE - units
    if extra:
        hidden = jnp.pad(hidden, ((0, 0), (0, extra)))
        w_down = jnp.pad(w_down, ((0, 0), (0, extra)))
    dma = pltpu.SemaphoreType.DMA
    vmem = pl.BlockSpec(memory_space=pltpu.VMEM)
    anywhere = pl.BlockSpec(memory_space=pl.ANY)
    hbm = pl.BlockSpec(memory_space=pltpu.HBM)
    grad_hidden, grad_weight = pl.pallas_call(
        functools.partial(kernel, (nodes, depth, chunks)),
        out_shape=(
            pltpu.VMEM((slots, chunks * WIDE), BF16),
            pltpu.VMEM((rows, chunks * WIDE), BF16),
        ),
        in_specs=[anywhere, anywhere, hbm, anywhere, anywhere],
        out_specs=(vmem, vmem),
        scratch_shapes=[
            pltpu.VMEM((slots,), F32),
            pltpu.SMEM((1,), jnp.int32),
            pltpu.VMEM((slots, half), BF16),
            pltpu.VMEM((nodes, slots, half), BF16),
            pltpu.VMEM((depth, 2, 2, rows, slots), BF16),
            pltpu.VMEM((depth, 2, rows, 2 * slots), BF16),
            pltpu.VMEM((2 * slots, chunks * WIDE), BF16),
            pltpu.VMEM((SLOTS, model, WIDE), BF16),
            pltpu.VMEM((chunks - 1, depth, 2, rows, WIDE), BF16),
            pltpu.VMEM((chunks - 1, depth, rows, WIDE), BF16),
            pltpu.VMEM((chunks - 1, depth, 2, rows, WIDE), BF16),
            pltpu.VMEM((chunks - 1, depth, 2, rows, WIDE), BF16),
            pltpu.VMEM((1, depth, 2, 2 * rows, WIDE), BF16),
            pltpu.VMEM((1, depth, 2 * rows, WIDE), BF16),
            pltpu.VMEM((1, depth, 2, 2 * rows, WIDE), BF16),
            pltpu.VMEM((1, depth, 2, 2 * rows, WIDE), BF16),
            pltpu.VMEM((rows, WIDE), BF16),
            dma((3,)),
            dma((3,)),
            dma((SLOTS,)),
            dma((nodes,)),
            dma((nodes,)),
            dma((nodes,)),
            dma((nodes,)),
            dma((near,)),
            dma((near,)),
            dma((nodes, near)),
            dma((nodes, near)),
            dma((chunks,)),
            dma((chunks,)),
            dma((chunks, depth)),
            dma((chunks, depth)),
            dma((chunks, depth)),
            dma((chunks, depth)),
            dma((chunks, depth)),
            dma((chunks, depth)),
        ]
        + [dma((1, depth))] * 6
        + [dma(())] * 2,
        compiler_params=pltpu.CompilerParams(
            collective_id=0, has_side_effects=True, vmem_limit_bytes=54 * 1024 * 1024
        ),
    )(grad_out, gate_prob, slot_counts, hidden, w_down)
    return pl.pallas_call(
        functools.partial(store, 3),
        out_shape=(
            jax.ShapeDtypeStruct((slots, units), BF16),
            jax.ShapeDtypeStruct((rows, units), BF16),
        ),
        in_specs=[anywhere, anywhere],
        out_specs=(anywhere, anywhere),
        scratch_shapes=[dma((4,))],
        compiler_params=pltpu.CompilerParams(vmem_limit_bytes=8 * 1024 * 1024),
    )(grad_hidden, grad_weight)


def solution(mesh):
    return jax.shard_map(
        body,
        mesh=mesh,
        in_specs=(P("grp", "node"), P("grp"), P("grp", "node"), P(None, "node"), P("grp")),
        out_specs=(P("grp", "node"), P("grp", "node")),
        check_vma=False,
    )
```
